32 devices in a mesh: row: 8 (over y, x, core), col: 4 (over z).
Axes of the slice: x: 2, y: 2, z: 4, core: 2. Of those that a mesh axis runs over, the one named last changes fastest.
Arguments:
- velocity: float32 [3, 2, 128, 256, 256], P(None, None, 'row', 'col'), may hold values from -7.5 to 7.5
- accumulator: float32 [3, 2, 128, 256, 256], P(None, None, 'row', 'col'), may hold values from -6 to 6
- remesh_flag: int32 [128], P('row'), may hold values 0 or 1
- remesh_shift: int32 [128], P('row'), may hold values from -128 to 127
- viscosity: float32 [1], replicated, may hold values from 0.0003 to 0.0015
- shear: float32 [1], replicated, may hold values from 8 to 20
- clock: float32 [1], replicated, may hold values from 0 to 0.05
- step: float32 [1], replicated, may hold values from 0.004 to 0.01
Outputs:
- new_velocity: float32 [3, 2, 128, 256, 256], P(None, None, 'row', 'col')
- new_accumulator: float32 [3, 2, 128, 256, 256], P(None, None, 'row', 'col')
- spectra: float32 [2, 128], P(None, 'row')
The draws below stay inside these ranges and needn't reach their ends.
All inputs are finite; a program needn't handle non-finite values. No bound on the sum of `remesh_flag` on one device may be relied on, other than what follows from the above.
Results may differ from the reference program's by a relative error of at most 0.0001.
Values sent between devices are 32-bit elements; how exact they have to be, the bound alone decides.
No kernel may reach another device: no remote copies, remote signals or barrier semaphores. Data moves between devices by JAX's collectives and lax.ppermute only.
A program may use at most 192 MiB of HBM per device.

```python
import math
import jax
import jax.numpy as jnp

NX = 256
NY = 256
NZ = 256
KX = 128


def draw_velocity(key, part):
    first_key = jax.random.fold_in(jax.random.fold_in(key, 11), 0)
    sample = jnp.clip(jax.random.normal(first_key, (3, 2, KX, NZ, NY), jnp.float32), -4.0, 4.0)
    correlated = sample.at[1].add(-0.6 * sample[0])
    return correlated


def set_ends(entries, stream_key, smallest, top_value):
    shape = entries.shape
    spot = [jax.random.randint(jax.random.fold_in(stream_key, axis), (), 0, shape[axis]) for axis in range(len(shape))]
    entries = entries.at[tuple(spot)].set(smallest)
    longest = shape.index(max(shape))
    spot[longest] = (spot[longest] + 1) % shape[longest]
    return entries.at[tuple(spot)].set(top_value)


def block_levels(stream_key, extent, cuts, low, high):
    gain = 1.0
    for position, parts in cuts:
        heights = jax.random.uniform(jax.random.fold_in(jax.random.fold_in(stream_key, 6), position), (parts,), jnp.float32, low / len(cuts), high / len(cuts))
        gain = gain * jnp.repeat(jnp.exp(heights), extent[position] // parts).reshape((-1,) + (1,) * (len(extent) - 1 - position))
    return gain


def gaussian(key, shape, width, bound, cuts=(), held_as=jnp.bfloat16):
    values = width * jax.random.normal(key, shape, jnp.float32)
    if cuts:
        values = values * block_levels(key, shape, cuts, -0.22, 0.18)
    return jnp.clip(values, -bound, bound).astype(held_as)


def setup_inputs(seed: int = 0) -> dict:
    key_list = jax.random.split(jax.random.key(seed), 9)
    return {
        "velocity": draw_velocity(jax.random.fold_in(key_list[8], 71), 0),
        "accumulator": gaussian(key_list[1], (3, 2, KX, NZ, NY), 1.0, 6.0, ((2, 8), (3, 4)), jnp.float32),
        "remesh_flag": set_ends((jax.random.randint(key_list[2], (KX,), 0, 2) < 1).astype(jnp.int32), jax.random.fold_in(key_list[2], 1), 0, 1),
        "remesh_shift": set_ends(jax.random.randint(key_list[3], (KX,), 0 - NY // 2, NY // 2), jax.random.fold_in(key_list[3], 1), 0 - NY // 2, (NY // 2) - 1).astype(jnp.int32),
        "viscosity": jnp.clip(jnp.exp(jax.random.uniform(key_list[4], (1,), jnp.float32, math.log(0.0003), math.log(0.0015))), 0.0003, 0.0015),
        "shear": jnp.clip(jax.random.uniform(key_list[5], (1,), jnp.float32, 8.0, 20.0), 8.0, 20.0),
        "clock": jnp.clip(jax.random.uniform(key_list[6], (1,), jnp.float32, 0.0, 0.05), 0.0, 0.05),
        "step": jnp.clip(jax.random.uniform(key_list[7], (1,), jnp.float32, 0.004, 0.01), 0.004, 0.01),
    }


def signed_index(positions, period):
    return jnp.where(2 * positions < period, positions, positions - period)


def roll_rows(field, amounts):
    def shift_row(row_data, amount_one):
        return jnp.roll(row_data, -amount_one, axis=-1)
    return jax.vmap(shift_row, in_axes=(2, 0), out_axes=2)(field, amounts)


def project(real_part, imag_part, wave_vector, inverse_square):
    along_real = (wave_vector[0] * real_part[0] + wave_vector[1] * real_part[1] + wave_vector[2] * real_part[2]) * inverse_square
    along_imag = (wave_vector[0] * imag_part[0] + wave_vector[1] * imag_part[1] + wave_vector[2] * imag_part[2]) * inverse_square
    return (jnp.stack([real_part[number] - wave_vector[number] * along_real for number in range(3)]),
            jnp.stack([imag_part[number] - wave_vector[number] * along_imag for number in range(3)]))


def cross_product(first_one, second_one):
    return jnp.stack([first_one[1] * second_one[2] - first_one[2] * second_one[1],
                      first_one[2] * second_one[0] - first_one[0] * second_one[2],
                      first_one[0] * second_one[1] - first_one[1] * second_one[0]])


def to_grid(real_part, imag_part):
    weights = jnp.where(jnp.arange(KX) == 0, 1.0, 2.0).astype(jnp.float32)[:, None, None]
    result_list = []
    for number in range(3):
        half = weights * (real_part[number] + 1j * imag_part[number])
        full = jnp.zeros((NX, NZ, NY), half.dtype).at[:KX].set(half)
        result_list.append(jnp.real(jnp.fft.ifftn(full, norm="ortho")))
    return jnp.stack(result_list)


def reference(velocity, accumulator, remesh_flag, remesh_shift, viscosity, shear, clock, step):
    offset = remesh_flag * remesh_shift
    remeshed = roll_rows(velocity, offset)
    carried = roll_rows(accumulator, offset)
    lattice_x = jnp.arange(KX, dtype=jnp.int32)
    lattice_z = signed_index(jnp.arange(NZ, dtype=jnp.int32), NZ)
    lattice_y = signed_index(jnp.arange(NY, dtype=jnp.int32), NY)
    wave_x = lattice_x.astype(jnp.float32)[:, None, None]
    wave_z = lattice_z.astype(jnp.float32)[None, :, None]
    wave_y = lattice_y.astype(jnp.float32)[None, None, :] - shear[0] * clock[0] * wave_x
    wave_vector = (wave_x, wave_y, wave_z)
    square_wave = wave_x * wave_x + wave_y * wave_y + wave_z * wave_z
    inverse_square = 1.0 / jnp.maximum(square_wave, 1.0)
    dealias_mask = ((3 * lattice_x < NX)[:, None, None] & (3 * jnp.abs(lattice_z) < NZ)[None, :, None]
                    & (3 * jnp.abs(lattice_y) < NY)[None, None, :]).astype(jnp.float32)
    solen_real, solen_imag = project(remeshed[:, 0], remeshed[:, 1], wave_vector, inverse_square)
    smooth_real = dealias_mask * solen_real
    smooth_imag = dealias_mask * solen_imag
    vort_real = -cross_product(wave_vector, smooth_imag)
    vort_imag = cross_product(wave_vector, smooth_real)
    flow_grid = to_grid(smooth_real, smooth_imag)
    swirl_grid = to_grid(vort_real, vort_imag)
    lamb_grid = cross_product(flow_grid, swirl_grid)
    lamb_hat = [jnp.fft.fftn(lamb_grid[number], norm="ortho")[:KX] for number in range(3)]
    hat_real = dealias_mask * jnp.stack([jnp.real(spectrum) for spectrum in lamb_hat])
    hat_imag = dealias_mask * jnp.stack([jnp.imag(spectrum) for spectrum in lamb_hat])
    proj_real, proj_imag = project(hat_real, hat_imag, wave_vector, inverse_square)
    shear_rate = shear[0]
    viscous_rate = viscosity[0]
    coupling = 2.0 * shear_rate * wave_x * inverse_square

    def tendency(projected, state):
        term_list = [projected[number] + coupling * wave_vector[number] * state[1] - viscous_rate * square_wave * state[number] for number in range(3)]
        term_list[0] = term_list[0] - shear_rate * state[1]
        return jnp.stack(term_list)

    tendencies = jnp.stack([tendency(proj_real, remeshed[:, 0]), tendency(proj_imag, remeshed[:, 1])], axis=1)
    new_accumulator = (-5.0 / 9.0) * carried + step[0] * tendencies
    new_velocity = remeshed + (15.0 / 16.0) * new_accumulator
    stress = jnp.sum(remeshed[0, 0] * remeshed[1, 0] + remeshed[0, 1] * remeshed[1, 1], axis=(1, 2)) / (NY * NZ)
    energy = jnp.sum(remeshed * remeshed, axis=(0, 1))
    dissipation = 2.0 * viscous_rate * jnp.sum(square_wave * energy, axis=(1, 2)) / (NY * NZ)
    return new_velocity, new_accumulator, jnp.stack([stress, dissipation])
```

```python
import functools
import math

import jax
import jax.numpy as jnp
import numpy as np
from jax import lax
from jax.experimental import pallas as pl
from jax.experimental.pallas import tpu as pltpu
from jax.sharding import PartitionSpec as P

F32 = jnp.float32
BF16 = jnp.bfloat16
VMEM_LIMIT = 56 * 1024 * 1024


def signed_index(positions, period):
    return jnp.where(2 * positions < period, positions, positions - period)


def roll_rows(field, amounts):

    def shift_row(row_data, amount_one):
        return jnp.roll(row_data, -amount_one, axis=-1)

    return jax.vmap(shift_row, in_axes=(2, 0), out_axes=2)(field, amounts)


def dft_tables(period):
    positions = jnp.arange(period, dtype=jnp.int32)
    product = positions[:, None] * positions[None, :] % period
    angles = product.astype(jnp.float32) * (2.0 * math.pi / period)
    factor = 1.0 / math.sqrt(period)
    return (jnp.cos(angles) * factor, jnp.sin(angles) * factor)


def product_high(formula, first_arg, second_arg):
    return jnp.einsum(formula, first_arg, second_arg, precision=lax.Precision.HIGHEST)


def rotate(left_side, right_side, output, real_part, imag_part, cosine_table, sine_table, backward):
    stacked = jnp.stack([real_part, imag_part])
    if backward:
        block_table = jnp.stack(
            [jnp.stack([cosine_table, sine_table]), jnp.stack([-sine_table, cosine_table])]
        )
    else:
        block_table = jnp.stack(
            [jnp.stack([cosine_table, -sine_table]), jnp.stack([sine_table, cosine_table])]
        )
    result = product_high(
        "s" + left_side + ",st" + right_side + "->t" + output, stacked, block_table
    )
    return (result[0], result[1])


def project(real_part, imag_part, wave_vector, inverse_square):
    along_real = (
        wave_vector[0] * real_part[0]
        + wave_vector[1] * real_part[1]
        + wave_vector[2] * real_part[2]
    ) * inverse_square
    along_imag = (
        wave_vector[0] * imag_part[0]
        + wave_vector[1] * imag_part[1]
        + wave_vector[2] * imag_part[2]
    ) * inverse_square
    return (
        jnp.stack([real_part[number] - wave_vector[number] * along_real for number in range(3)]),
        jnp.stack([imag_part[number] - wave_vector[number] * along_imag for number in range(3)]),
    )


def cross_product(first_one, second_one):
    return jnp.stack(
        [
            first_one[1] * second_one[2] - first_one[2] * second_one[1],
            first_one[2] * second_one[0] - first_one[0] * second_one[2],
            first_one[0] * second_one[1] - first_one[1] * second_one[0],
        ]
    )


def to_physical(real_part, imag_part, tables_all):
    (cos_y, sin_y), (cos_x, sin_x), (cos_z, sin_z) = tables_all
    row_count = lax.axis_size("row")
    col_count = lax.axis_size("col")
    fields, width_x, width_z, full_y = real_part.shape
    block_y = full_y // row_count
    half_x = width_x * row_count
    full_x = cos_x.shape[0]
    block_x = full_x // col_count
    full_z = width_z * col_count
    shape_y = (full_y, row_count, block_y)
    first_real, first_imag = rotate(
        "fabc",
        "cpq",
        "fpabq",
        real_part,
        imag_part,
        cos_y.reshape(shape_y),
        sin_y.reshape(shape_y),
        True,
    )
    flat_shape = (fields, row_count, width_x, width_z * block_y)
    second_real, second_imag = (
        lax.all_to_all(
            first_real.reshape(flat_shape), "row", split_axis=1, concat_axis=2, tiled=True
        ),
        lax.all_to_all(
            first_imag.reshape(flat_shape), "row", split_axis=1, concat_axis=2, tiled=True
        ),
    )
    deep_shape = (fields, half_x, width_z, block_y)
    weights = jnp.where(jnp.arange(half_x) == 0, 1.0, 2.0).astype(jnp.float32)[:, None]
    shape_x = (half_x, col_count, block_x)
    cos_half = (weights * cos_x[:half_x]).reshape(shape_x)
    sin_half = (weights * sin_x[:half_x]).reshape(shape_x)
    third_real, third_imag = rotate(
        "fkzy",
        "kpq",
        "fpzyq",
        second_real.reshape(deep_shape),
        second_imag.reshape(deep_shape),
        cos_half,
        sin_half,
        True,
    )
    flat_shape = (fields, col_count, 1, width_z * block_y * block_x)
    fourth_real, fourth_imag = (
        lax.all_to_all(
            third_real.reshape(flat_shape), "col", split_axis=1, concat_axis=2, tiled=True
        ),
        lax.all_to_all(
            third_imag.reshape(flat_shape), "col", split_axis=1, concat_axis=2, tiled=True
        ),
    )
    deep_shape = (fields, col_count, width_z, block_y, block_x)
    shape_z = (col_count, width_z, full_z)
    stacked = jnp.stack([fourth_real.reshape(deep_shape), fourth_imag.reshape(deep_shape)])
    z_table = jnp.stack([cos_z.reshape(shape_z), -sin_z.reshape(shape_z)])
    return product_high("sfpkyq,spkn->fyqn", stacked, z_table)


def to_spectral(physical, tables_all, half_x):
    (cos_y, sin_y), (cos_x, sin_x), (cos_z, sin_z) = tables_all
    row_count = lax.axis_size("row")
    col_count = lax.axis_size("col")
    fields, block_y, block_x, full_z = physical.shape
    width_z = full_z // col_count
    width_x = half_x // row_count
    full_y = block_y * row_count
    shape_z = (full_z, col_count, width_z)
    z_table = jnp.stack([cos_z.reshape(shape_z), -sin_z.reshape(shape_z)])
    first_both = product_high("fyqn,tnpk->tfpkyq", physical, z_table)
    first_real, first_imag = (first_both[0], first_both[1])
    flat_shape = (fields, col_count, 1, width_z * block_y * block_x)
    second_real, second_imag = (
        lax.all_to_all(
            first_real.reshape(flat_shape), "col", split_axis=1, concat_axis=2, tiled=True
        ),
        lax.all_to_all(
            first_imag.reshape(flat_shape), "col", split_axis=1, concat_axis=2, tiled=True
        ),
    )
    deep_shape = (fields, col_count, width_z, block_y, block_x)
    shape_x = (col_count, block_x, row_count, width_x)
    third_real, third_imag = rotate(
        "fpkyq",
        "pqmr",
        "fmrky",
        second_real.reshape(deep_shape),
        second_imag.reshape(deep_shape),
        cos_x[:, :half_x].reshape(shape_x),
        sin_x[:, :half_x].reshape(shape_x),
        False,
    )
    flat_shape = (fields, row_count, 1, width_x * width_z * block_y)
    fourth_real, fourth_imag = (
        lax.all_to_all(
            third_real.reshape(flat_shape), "row", split_axis=1, concat_axis=2, tiled=True
        ),
        lax.all_to_all(
            third_imag.reshape(flat_shape), "row", split_axis=1, concat_axis=2, tiled=True
        ),
    )
    deep_shape = (fields, row_count, width_x, width_z, block_y)
    shape_y = (row_count, block_y, full_y)
    return rotate(
        "fparq",
        "pqn",
        "farn",
        fourth_real.reshape(deep_shape),
        fourth_imag.reshape(deep_shape),
        cos_y.reshape(shape_y),
        sin_y.reshape(shape_y),
        False,
    )


def many_physical(real_part, imag_part, tables_all):
    return jnp.concatenate(
        [
            to_physical(real_part[number : number + 1], imag_part[number : number + 1], tables_all)
            for number in range(real_part.shape[0])
        ]
    )


def many_spectral(physical, tables_all, half_x):
    result_list = [
        to_spectral(physical[number : number + 1], tables_all, half_x)
        for number in range(physical.shape[0])
    ]
    return (
        jnp.concatenate([entry[0] for entry in result_list]),
        jnp.concatenate([entry[1] for entry in result_list]),
    )


def body(velocity, accumulator, remesh_flag, remesh_shift, viscosity, shear, clock, step):
    width_x = velocity.shape[2]
    width_z = velocity.shape[3]
    full_y = velocity.shape[4]
    half_x = width_x * lax.axis_size("row")
    NX, NY, NZ = 2 * half_x, full_y, width_z * lax.axis_size("col")
    offset = remesh_flag * remesh_shift
    remeshed = roll_rows(velocity, offset)
    carried = roll_rows(accumulator, offset)
    lattice_x = lax.axis_index("row") * width_x + jnp.arange(width_x, dtype=jnp.int32)
    col_index = lax.axis_index("col") * width_z + jnp.arange(width_z, dtype=jnp.int32)
    lattice_z = signed_index(col_index, NZ)
    lattice_y = signed_index(jnp.arange(full_y, dtype=jnp.int32), NY)
    wave_x = lattice_x.astype(jnp.float32)[:, None, None]
    wave_z = lattice_z.astype(jnp.float32)[None, :, None]
    wave_y = lattice_y.astype(jnp.float32)[None, None, :] - shear[0] * clock[0] * wave_x
    wave_vector = (wave_x, wave_y, wave_z)
    square_wave = wave_x * wave_x + wave_y * wave_y + wave_z * wave_z
    inverse_square = 1.0 / jnp.maximum(square_wave, 1.0)
    dealias_mask = (
        (3 * lattice_x < NX)[:, None, None]
        & (3 * jnp.abs(lattice_z) < NZ)[None, :, None]
        & (3 * jnp.abs(lattice_y) < NY)[None, None, :]
    ).astype(jnp.float32)
    shear_rate = shear[0]
    viscous_rate = viscosity[0]
    stress_part = jnp.sum(
        remeshed[0, 0] * remeshed[1, 0] + remeshed[0, 1] * remeshed[1, 1], axis=(1, 2)
    )
    energy = jnp.sum(remeshed * remeshed, axis=(0, 1))
    dissipation_part = jnp.sum(square_wave * energy, axis=(1, 2))
    stress_total, dissipation_total = lax.psum((stress_part, dissipation_part), "col")
    solen_real, solen_imag = project(remeshed[:, 0], remeshed[:, 1], wave_vector, inverse_square)
    smooth_real = dealias_mask * solen_real
    smooth_imag = dealias_mask * solen_imag
    tables_all = (dft_tables(NY), dft_tables(NX), dft_tables(NZ))
    vort_real = -cross_product(wave_vector, smooth_imag)
    vort_imag = cross_product(wave_vector, smooth_real)
    both_real = jnp.concatenate([smooth_real, vort_real])
    both_imag = jnp.concatenate([smooth_imag, vort_imag])
    physical = many_physical(both_real, both_imag, tables_all)
    lamb_grid = cross_product(physical[:3], physical[3:])
    modes_real, modes_imag = many_spectral(lamb_grid, tables_all, half_x)
    hat_real = dealias_mask * modes_real
    hat_imag = dealias_mask * modes_imag
    proj_real, proj_imag = project(hat_real, hat_imag, wave_vector, inverse_square)
    coupling = 2.0 * shear_rate * wave_x * inverse_square

    def tendency(projected, state):
        term_list = [
            projected[number]
            + coupling * wave_vector[number] * state[1]
            - viscous_rate * square_wave * state[number]
            for number in range(3)
        ]
        term_list[0] = term_list[0] - shear_rate * state[1]
        return jnp.stack(term_list)

    tendencies = jnp.stack(
        [tendency(proj_real, remeshed[:, 0]), tendency(proj_imag, remeshed[:, 1])], axis=1
    )
    new_accumulator = -5.0 / 9.0 * carried + step[0] * tendencies
    new_velocity = remeshed + 15.0 / 16.0 * new_accumulator
    stress = stress_total / (NY * NZ)
    dissipation = 2.0 * viscous_rate * dissipation_total / (NY * NZ)
    return (new_velocity, new_accumulator, jnp.stack([stress, dissipation]))


def kappa(n):
    index = np.arange(n)
    return np.where(2 * index < n, index, index - n)


def angle(rows, cols, n):
    product = np.outer(rows, cols) % n
    return np.cos(2 * np.pi * product / n) / math.sqrt(n), np.sin(2 * np.pi * product / n) / math.sqrt(n)


def halves(table):
    table = np.asarray(table, np.float32)
    high = table.astype(jnp.bfloat16)
    low = (table - high.astype(np.float32)).astype(jnp.bfloat16)
    return jnp.asarray(high), jnp.asarray(low)


def split(x):
    high = x.astype(BF16)
    return high, (x - high.astype(F32)).astype(BF16)


def dot(a, b, dims):
    return lax.dot_general(a, b, (dims, ((), ())), preferred_element_type=F32)


class Sizes:
    def __init__(self, rows, cols, width_x, width_z, full_y):
        self.rows, self.cols = rows, cols
        self.width_x, self.width_z = width_x, width_z
        self.half_x = width_x * rows
        self.full_x = 2 * self.half_x
        self.full_z = width_z * cols
        self.full_y = full_y
        self.block_y = full_y // (rows * cols)
        live = (self.full_x - 1) // 3 + 1
        self.live_x = -(-live // 8) * 8
        self.lanes = 2 * width_z

    def fits(self):
        return (
            self.block_y == 8
            and self.lanes == 128
            and self.full_y % 128 == 0
            and self.full_z % 128 == 0
            and self.full_x % 128 == 0
            and self.width_x % 2 == 0
            and self.rows & (self.rows - 1) == 0
            and self.cols & (self.cols - 1) == 0
        )


def constant_tables(s):
    c, n = angle(np.arange(s.full_y), np.arange(s.full_y), s.full_y)
    y_back = np.concatenate([c, -n], axis=1)
    y_fore = np.concatenate([c, n], axis=1)
    live = np.arange(s.live_x)
    weight = np.where(live == 0, 1.0, 2.0) * (3 * live < s.full_x)
    c, n = angle(np.arange(s.full_x), live, s.full_x)
    x_back = np.concatenate([c * weight, -n * weight], axis=1)
    x_fore = np.concatenate([c.T, -n.T], axis=0)
    c, n = angle(np.arange(s.full_z), np.arange(s.full_z), s.full_z)
    c3, n3 = c.reshape(s.cols, s.width_z, s.full_z), n.reshape(s.cols, s.width_z, s.full_z)
    z_back = np.concatenate(
        [np.concatenate([c3, n3], axis=2), np.concatenate([-n3, c3], axis=2)], axis=1
    )
    ct, nt = c3.transpose(0, 2, 1), n3.transpose(0, 2, 1)
    z_fore = np.concatenate(
        [np.concatenate([ct, -nt], axis=2), np.concatenate([nt, ct], axis=2)], axis=1
    )
    return [halves(t) for t in (y_back, y_fore, x_back, x_fore, z_back, z_fore)]


def whole(shape):
    return pl.BlockSpec(shape, lambda *_: (0,) * len(shape))


def waves(s, kx, col, shear_clock):
    plane = (s.width_z, s.full_y)
    iz = lax.broadcasted_iota(jnp.int32, plane, 0) + col * s.width_z
    iz = jnp.where(2 * iz < s.full_z, iz, iz - s.full_z)
    iy = lax.broadcasted_iota(jnp.int32, plane, 1)
    iy = jnp.where(2 * iy < s.full_y, iy, iy - s.full_y)
    k0 = kx.astype(F32)
    k1 = iy.astype(F32) - shear_clock * k0
    k2 = iz.astype(F32)
    ksq = k0 * k0 + k1 * k1 + k2 * k2
    inverse = 1.0 / jnp.maximum(ksq, 1.0)
    inside = (3 * jnp.abs(iz) < s.full_z) & (3 * jnp.abs(iy) < s.full_y) & (3 * kx < s.full_x)
    return k0, k1, k2, ksq, inverse, inside.astype(F32)


def rolled(s, ref, j, amount):
    flat = jnp.concatenate([ref[c, p, j] for c in range(3) for p in range(2)], axis=0)
    flat = pltpu.roll(flat, lax.rem(s.full_y - amount, s.full_y), 1)
    w = s.width_z
    return [[flat[(2 * c + p) * w : (2 * c + p + 1) * w] for p in range(2)] for c in range(3)]


def head_kernel(s, ints, floats, vel, yh, yl, *outs):
    fields, sums = outs[:3], outs[3]
    row, col = ints[0], ints[1]
    step = pl.program_id(0)
    right = [[], [], []]
    for j in range(2):
        local = 2 * step + j
        kx = row * s.width_x + local
        v = rolled(s, vel, j, ints[2 + local])
        k0, k1, k2, ksq, inverse, mask = waves(s, kx, col, floats[0])
        stress = v[0][0] * v[1][0] + v[0][1] * v[1][1]
        energy = sum(v[c][p] * v[c][p] for c in range(3) for p in range(2))
        fold = lambda a: jnp.sum(a.reshape(s.width_z // 8, 8, s.full_y), axis=0)
        sums[j, 0] = fold(stress)
        sums[j, 1] = fold(ksq * energy)
        along = [(k0 * v[0][p] + k1 * v[1][p] + k2 * v[2][p]) * inverse for p in range(2)]
        for c, k in enumerate((k0, k1, k2)):
            (rh, rl), (ih, il) = [split(mask * (v[c][p] - k * along[p])) for p in range(2)]
            right[c].append(jnp.concatenate([rh, ih, rl, il, rh, ih], axis=1))
            right[c].append(jnp.concatenate([ih, -rh, il, -rl, ih, -rh], axis=1))
    left = jnp.concatenate([yh[...], yh[...], yl[...]], axis=1)
    for c in range(3):
        out = dot(left, jnp.concatenate(right[c], axis=0), ((1,), (1,)))
        for r in range(s.rows):
            for q in range(s.cols):
                at = (r * s.cols + q) * 8
                for j in range(2):
                    fields[c][r, q ^ col, j] = out[at : at + 8, j * 128 : (j + 1) * 128]


def head(s, ints, floats, velocity, table):
    y2 = (s.full_y, 2 * s.full_y)
    piece = (s.rows, s.cols, s.width_x, 8, s.lanes)
    return pl.pallas_call(
        functools.partial(head_kernel, s),
        grid=(s.width_x // 2,),
        in_specs=[
            pl.BlockSpec(memory_space=pltpu.SMEM),
            pl.BlockSpec(memory_space=pltpu.SMEM),
            pl.BlockSpec((3, 2, 2, s.width_z, s.full_y), lambda i: (0, 0, i, 0, 0)),
            whole(y2),
            whole(y2),
        ],
        out_specs=[pl.BlockSpec((s.rows, s.cols, 2, 8, s.lanes), lambda i: (0, 0, i, 0, 0))] * 3
        + [pl.BlockSpec((2, 2, 8, s.full_y), lambda i: (i, 0, 0, 0))],
        out_shape=[jax.ShapeDtypeStruct(piece, F32)] * 3
        + [jax.ShapeDtypeStruct((s.width_x, 2, 8, s.full_y), F32)],
        compiler_params=pltpu.CompilerParams(vmem_limit_bytes=VMEM_LIMIT),
        name="head",
    )(ints, floats, velocity, *table)


def stack3(a):
    high, low = split(a)
    return high, low


def grid_kernel(s, ints, *refs):
    pieces, (zh, zl, xh, xl, out, mid) = refs[: s.cols], refs[s.cols :]
    col = ints[1]
    rows = s.live_x * 8
    step = rows // 4
    zt = jnp.concatenate(
        [zh[q ^ col] for q in range(s.cols)] * 2 + [zl[q ^ col] for q in range(s.cols)], axis=0
    )

    def along_z(i, carry):
        at = pl.multiple_of(i * (step // 8), step // 8)
        parts = [split(p[pl.ds(at, step // 8)].reshape(step, s.lanes)) for p in pieces]
        highs, lows = [h for h, _ in parts], [l for _, l in parts]
        left = jnp.concatenate(highs + lows + highs, axis=1)
        full = dot(left, zt, ((1,), (0,)))
        for t in range(2 * s.full_z // 128):
            mid[t, pl.ds(pl.multiple_of(i * step, step), step)] = full[:, t * 128 : (t + 1) * 128]
        return carry

    lax.fori_loop(0, 4, along_z, 0)
    xt = jnp.concatenate([xh[...], xh[...], xl[...]], axis=1)

    def along_x(y, carry):
        tiles = [mid[t, pl.ds(y, s.live_x, stride=8)] for t in range(2 * s.full_z // 128)]
        half = s.full_z // 128
        both = [jnp.concatenate(tiles[:half], axis=1), jnp.concatenate(tiles[half:], axis=1)]
        high, low = split(jnp.concatenate(both, axis=0))
        out[y] = dot(xt, jnp.concatenate([high, low, high], axis=0), ((1,), (0,)))
        return carry

    lax.fori_loop(0, 8, along_x, 0)


def to_grid(s, ints, pieces, z_table, x_table):
    rows = s.live_x * 8
    return pl.pallas_call(
        functools.partial(grid_kernel, s),
        in_specs=[pl.BlockSpec(memory_space=pltpu.SMEM)]
        + [pl.BlockSpec(memory_space=pltpu.VMEM)] * (s.cols + 4),
        out_specs=pl.BlockSpec(memory_space=pltpu.VMEM),
        out_shape=jax.ShapeDtypeStruct((8, s.full_x, s.full_z), F32),
        scratch_shapes=[pltpu.VMEM((2 * s.full_z // 128, rows, 128), F32)],
        compiler_params=pltpu.CompilerParams(vmem_limit_bytes=VMEM_LIMIT),
        name="to_grid",
    )(ints, *pieces, *z_table, *x_table)


def turn(s, rows, base, kz):
    k0 = ((lax.broadcasted_iota(jnp.int32, (rows, s.lanes), 0) + base) // 8).astype(F32)
    square = k0 * k0 + kz * kz
    scale = lax.rsqrt(jnp.maximum(square, 1.0))
    return jnp.where(square > 0, k0 * scale, 1.0), kz * scale


def back_kernel(s, which, ints, *refs):
    number = 2 if which == 0 else 3
    u, (xh, xl, zh, zl) = refs[:3], refs[3:7]
    outs, mids = refs[7 : 7 + 2 * s.cols], refs[7 + 2 * s.cols :]
    col = ints[1]
    xt = jnp.concatenate([xh[...], xh[...], xl[...]], axis=1)

    def along_x(y, carry):
        a, b, c = u[0][y], u[1][y], u[2][y]
        if which == 0:
            terms = [a * b, b * c]
        else:
            cc = c * c
            terms = [a * a - cc, b * b - cc, a * c]
        for mid, term in zip(mids, terms):
            high, low = split(term)
            out = dot(xt, jnp.concatenate([high, low, high], axis=0), ((1,), (0,)))
            half = s.full_z // 128
            for t in range(2 * half):
                p, at = t // half, (t % half) * 128
                tile = out[p * s.live_x : (p + 1) * s.live_x, at : at + 128]
                mid[t, pl.ds(y, s.live_x, stride=8)] = tile
        return carry

    lax.fori_loop(0, 8, along_x, 0)
    rows = s.live_x * 8
    step = rows // 4
    zt = [jnp.concatenate([zh[q ^ col], zh[q ^ col], zl[q ^ col]], axis=0) for q in range(s.cols)]
    zt = jnp.concatenate(zt, axis=1)

    def along_z(i, carry):
        at = pl.multiple_of(i * step, step)
        done = []
        for mid in mids:
            high, low = split(
                jnp.concatenate([mid[t, pl.ds(at, step)] for t in range(2 * s.full_z // 128)], axis=1)
            )
            done.append(dot(jnp.concatenate([high, low, high], axis=1), zt, ((1,), (0,))))
        for q in range(s.cols):
            lane = lax.broadcasted_iota(jnp.int32, (step, s.lanes), 1)
            iz = lax.rem(lane, s.width_z) + (q ^ col) * s.width_z
            kz = jnp.where(2 * iz < s.full_z, iz, iz - s.full_z).astype(F32)
            cosine, sine = turn(s, step, i * step, kz)
            part = [d[:, q * s.lanes : (q + 1) * s.lanes] for d in done]
            if which == 0:
                first = sine * part[0] - cosine * part[1]
                second = cosine * part[0] + sine * part[1]
            else:
                first = cosine * sine * part[0] + (sine * sine - cosine * cosine) * part[2]
                second = part[1] - cosine * (cosine * part[0] + 2.0 * sine * part[2])
            here = pl.ds(pl.multiple_of(i * (step // 8), step // 8), step // 8)
            shape = (step // 8, 8, s.lanes)
            outs[q][here] = first.reshape(shape)
            outs[s.cols + q][here] = second.reshape(shape)
        return carry

    lax.fori_loop(0, 4, along_z, 0)


def products(s, which, ints, fields, x_table, z_table):
    rows = s.live_x * 8
    number = 2 if which == 0 else 3
    piece = jax.ShapeDtypeStruct((s.live_x, 8, s.lanes), F32)
    out = pl.pallas_call(
        functools.partial(back_kernel, s, which),
        in_specs=[pl.BlockSpec(memory_space=pltpu.SMEM)] + [pl.BlockSpec(memory_space=pltpu.VMEM)] * 7,
        out_specs=[pl.BlockSpec(memory_space=pltpu.VMEM)] * (2 * s.cols),
        out_shape=[piece] * (2 * s.cols),
        scratch_shapes=[pltpu.VMEM((2 * s.full_z // 128, rows, 128), F32)] * number,
        compiler_params=pltpu.CompilerParams(vmem_limit_bytes=VMEM_LIMIT),
        name="products%d" % which,
    )(ints, *fields, *x_table, *z_table)
    return out[: s.cols], out[s.cols :]


def tail_kernel(s, ints, floats, vel, acc, fa, fb, fc, ff, yh, yl, new_vel, new_acc):
    row, col = ints[0], ints[1]
    local = pl.program_id(0)
    kx = row * s.width_x + local
    amount = ints[2 + local]
    right = jnp.concatenate([yh[...], yh[...], yl[...]], axis=0)
    modes = []
    for ref in (fa, fb, fc, ff):
        tiles = [ref[r, q ^ col, 0] for r in range(s.rows) for q in range(s.cols)]
        high, low = split(jnp.concatenate(tiles, axis=0).T)
        both = dot(jnp.concatenate([high, low, high], axis=1), right, ((1,), (0,)))
        w, n = s.width_z, s.full_y
        modes.append((both[:w, :n] + both[w:, n:], both[w:, :n] - both[:w, n:]))
    k0, k1, k2, ksq, inverse, mask = waves(s, kx, col, floats[0])
    flat = k0 * k0 + k2 * k2
    scale = lax.rsqrt(jnp.maximum(flat, 1.0))
    cosine, sine = jnp.where(flat > 0, k0 * scale, 1.0), k2 * scale
    kh = flat * scale
    lean = (flat - k1 * k1) * inverse
    cross = kh * k1 * inverse
    v = rolled(s, vel, 0, amount)
    old = rolled(s, acc, 0, amount)
    shear, viscosity, dt = floats[1], floats[2], floats[3]
    coupling = (2.0 * shear) * k0 * inverse
    for p in range(2):
        a, b, c, f = [m[1 - p] for m in modes]
        sign = mask if p == 0 else -mask
        qt = (kh * a + k1 * b) * sign
        qe = (lean * c + cross * f) * sign
        slope = qe * k1
        nonlinear = (qt * sine - slope * cosine, qe * kh, -(qt * cosine) - slope * sine)
        drive = coupling * v[1][p]
        for c3, k in enumerate((k0, k1, k2)):
            rate = nonlinear[c3] + k * drive - (viscosity * ksq) * v[c3][p]
            if c3 == 0:
                rate = rate - shear * v[1][p]
            fresh = (-5.0 / 9.0) * old[c3][p] + dt * rate
            new_acc[c3, p, 0] = fresh
            new_vel[c3, p, 0] = v[c3][p] + (15.0 / 16.0) * fresh


def tail(s, ints, floats, velocity, accumulator, fields, table):
    plane = pl.BlockSpec((3, 2, 1, s.width_z, s.full_y), lambda i: (0, 0, i, 0, 0))
    piece = pl.BlockSpec((s.rows, s.cols, 1, 8, s.lanes), lambda i: (0, 0, i, 0, 0))
    y2 = (s.full_y, 2 * s.full_y)
    shape = jax.ShapeDtypeStruct(velocity.shape, F32)
    return pl.pallas_call(
        functools.partial(tail_kernel, s),
        grid=(s.width_x,),
        in_specs=[pl.BlockSpec(memory_space=pltpu.SMEM)] * 2 + [plane] * 2 + [piece] * 4 + [whole(y2)] * 2,
        out_specs=[plane] * 2,
        out_shape=[shape] * 2,
        compiler_params=pltpu.CompilerParams(vmem_limit_bytes=VMEM_LIMIT),
        name="tail",
    )(ints, floats, velocity, accumulator, *fields, *table)


def col_exchange(s, pieces):
    out = [pieces[0]]
    for q in range(1, s.cols):
        out.append(lax.ppermute(pieces[q], "col", [(i, i ^ q) for i in range(s.cols)]))
    return out


def forward_field(s, field):
    got = lax.all_to_all(field, "row", 0, 0, tiled=True)
    pieces = [
        got[:, q].reshape(s.half_x, 8, s.lanes)[: s.live_x] for q in range(s.cols)
    ]
    return col_exchange(s, pieces)


def backward_field(s, pieces):
    got = col_exchange(s, pieces)
    spare = ((0, s.half_x - s.live_x), (0, 0), (0, 0))
    both = jnp.stack(
        [jnp.pad(p, spare).reshape(s.rows, s.width_x, 8, s.lanes) for p in got], axis=1
    )
    return lax.all_to_all(both, "row", 0, 0, tiled=True)


def tiled_body(s, velocity, accumulator, remesh_flag, remesh_shift, viscosity, shear, clock, step):
    y_back, y_fore, x_back, x_fore, z_back, z_fore = constant_tables(s)
    place = jnp.stack([lax.axis_index("row"), lax.axis_index("col")]).astype(jnp.int32)
    ints = jnp.concatenate([place, remesh_flag * remesh_shift])
    floats = jnp.concatenate([shear * clock, shear, viscosity, step])
    *spectral, sums = head(s, ints, floats, velocity, y_back)
    grid = [to_grid(s, ints, forward_field(s, f), z_back, x_back) for f in spectral]
    b, c = products(s, 0, ints, grid, x_fore, z_fore)
    a, f = products(s, 1, ints, grid, x_fore, z_fore)
    b, c, a, f = [backward_field(s, q) for q in (b, c, a, f)]
    new_velocity, new_accumulator = tail(
        s, ints, floats, velocity, accumulator, (a, b, c, f), y_fore
    )
    totals = lax.psum(jnp.sum(sums, axis=(2, 3)), "col") / (s.full_y * s.full_z)
    spectra = jnp.stack([totals[:, 0], 2.0 * viscosity[0] * totals[:, 1]])
    return new_velocity, new_accumulator, spectra


def solution(mesh):
    in_specs = (
        P(None, None, "row", "col", None),
        P(None, None, "row", "col", None),
        P("row"),
        P("row"),
        P(),
        P(),
        P(),
        P(),
    )
    out_specs = (
        P(None, None, "row", "col", None),
        P(None, None, "row", "col", None),
        P(None, "row"),
    )
    rows, cols = mesh.shape["row"], mesh.shape["col"]

    def local(velocity, *rest):
        s = Sizes(rows, cols, velocity.shape[2], velocity.shape[3], velocity.shape[4])
        run = functools.partial(tiled_body, s) if s.fits() else body
        return run(velocity, *rest)

    return jax.shard_map(local, mesh=mesh, in_specs=in_specs, out_specs=out_specs, check_vma=False)
```

```python
import functools
import math

import jax
import jax.numpy as jnp
import numpy as np
from jax import lax
from jax.experimental import pallas as pl
from jax.experimental.pallas import tpu as pltpu
from jax.sharding import PartitionSpec as P


F32 = jnp.float32
BF16 = jnp.bfloat16
VMEM_LIMIT = 56 * 1024 * 1024


def signed_index(positions, period):
    return jnp.where(2 * positions < period, positions, positions - period)


def roll_rows(field, amounts):

    def shift_row(row_data, amount_one):
        return jnp.roll(row_data, -amount_one, axis=-1)

    return jax.vmap(shift_row, in_axes=(2, 0), out_axes=2)(field, amounts)


def dft_tables(period):
    positions = jnp.arange(period, dtype=jnp.int32)
    product = positions[:, None] * positions[None, :] % period
    angles = product.astype(jnp.float32) * (2.0 * math.pi / period)
    factor = 1.0 / math.sqrt(period)
    return (jnp.cos(angles) * factor, jnp.sin(angles) * factor)


def product_high(formula, first_arg, second_arg):
    return jnp.einsum(formula, first_arg, second_arg, precision=lax.Precision.HIGHEST)


def rotate(left_side, right_side, output, real_part, imag_part, cosine_table, sine_table, backward):
    stacked = jnp.stack([real_part, imag_part])
    if backward:
        block_table = jnp.stack(
            [jnp.stack([cosine_table, sine_table]), jnp.stack([-sine_table, cosine_table])]
        )
    else:
        block_table = jnp.stack(
            [jnp.stack([cosine_table, -sine_table]), jnp.stack([sine_table, cosine_table])]
        )
    result = product_high(
        "s" + left_side + ",st" + right_side + "->t" + output, stacked, block_table
    )
    return (result[0], result[1])


def project(real_part, imag_part, wave_vector, inverse_square):
    along_real = (
        wave_vector[0] * real_part[0]
        + wave_vector[1] * real_part[1]
        + wave_vector[2] * real_part[2]
    ) * inverse_square
    along_imag = (
        wave_vector[0] * imag_part[0]
        + wave_vector[1] * imag_part[1]
        + wave_vector[2] * imag_part[2]
    ) * inverse_square
    return (
        jnp.stack([real_part[number] - wave_vector[number] * along_real for number in range(3)]),
        jnp.stack([imag_part[number] - wave_vector[number] * along_imag for number in range(3)]),
    )


def cross_product(first_one, second_one):
    return jnp.stack(
        [
            first_one[1] * second_one[2] - first_one[2] * second_one[1],
            first_one[2] * second_one[0] - first_one[0] * second_one[2],
            first_one[0] * second_one[1] - first_one[1] * second_one[0],
        ]
    )


def to_physical(real_part, imag_part, tables_all):
    (cos_y, sin_y), (cos_x, sin_x), (cos_z, sin_z) = tables_all
    row_count = lax.axis_size("row")
    col_count = lax.axis_size("col")
    fields, width_x, width_z, full_y = real_part.shape
    block_y = full_y // row_count
    half_x = width_x * row_count
    full_x = cos_x.shape[0]
    block_x = full_x // col_count
    full_z = width_z * col_count
    shape_y = (full_y, row_count, block_y)
    first_real, first_imag = rotate(
        "fabc",
        "cpq",
        "fpabq",
        real_part,
        imag_part,
        cos_y.reshape(shape_y),
        sin_y.reshape(shape_y),
        True,
    )
    flat_shape = (fields, row_count, width_x, width_z * block_y)
    second_real, second_imag = (
        lax.all_to_all(
            first_real.reshape(flat_shape), "row", split_axis=1, concat_axis=2, tiled=True
        ),
        lax.all_to_all(
            first_imag.reshape(flat_shape), "row", split_axis=1, concat_axis=2, tiled=True
        ),
    )
    deep_shape = (fields, half_x, width_z, block_y)
    weights = jnp.where(jnp.arange(half_x) == 0, 1.0, 2.0).astype(jnp.float32)[:, None]
    shape_x = (half_x, col_count, block_x)
    cos_half = (weights * cos_x[:half_x]).reshape(shape_x)
    sin_half = (weights * sin_x[:half_x]).reshape(shape_x)
    third_real, third_imag = rotate(
        "fkzy",
        "kpq",
        "fpzyq",
        second_real.reshape(deep_shape),
        second_imag.reshape(deep_shape),
        cos_half,
        sin_half,
        True,
    )
    flat_shape = (fields, col_count, 1, width_z * block_y * block_x)
    fourth_real, fourth_imag = (
        lax.all_to_all(
            third_real.reshape(flat_shape), "col", split_axis=1, concat_axis=2, tiled=True
        ),
        lax.all_to_all(
            third_imag.reshape(flat_shape), "col", split_axis=1, concat_axis=2, tiled=True
        ),
    )
    deep_shape = (fields, col_count, width_z, block_y, block_x)
    shape_z = (col_count, width_z, full_z)
    stacked = jnp.stack([fourth_real.reshape(deep_shape), fourth_imag.reshape(deep_shape)])
    z_table = jnp.stack([cos_z.reshape(shape_z), -sin_z.reshape(shape_z)])
    return product_high("sfpkyq,spkn->fyqn", stacked, z_table)


def to_spectral(physical, tables_all, half_x):
    (cos_y, sin_y), (cos_x, sin_x), (cos_z, sin_z) = tables_all
    row_count = lax.axis_size("row")
    col_count = lax.axis_size("col")
    fields, block_y, block_x, full_z = physical.shape
    width_z = full_z // col_count
    width_x = half_x // row_count
    full_y = block_y * row_count
    shape_z = (full_z, col_count, width_z)
    z_table = jnp.stack([cos_z.reshape(shape_z), -sin_z.reshape(shape_z)])
    first_both = product_high("fyqn,tnpk->tfpkyq", physical, z_table)
    first_real, first_imag = (first_both[0], first_both[1])
    flat_shape = (fields, col_count, 1, width_z * block_y * block_x)
    second_real, second_imag = (
        lax.all_to_all(
            first_real.reshape(flat_shape), "col", split_axis=1, concat_axis=2, tiled=True
        ),
        lax.all_to_all(
            first_imag.reshape(flat_shape), "col", split_axis=1, concat_axis=2, tiled=True
        ),
    )
    deep_shape = (fields, col_count, width_z, block_y, block_x)
    shape_x = (col_count, block_x, row_count, width_x)
    third_real, third_imag = rotate(
        "fpkyq",
        "pqmr",
        "fmrky",
        second_real.reshape(deep_shape),
        second_imag.reshape(deep_shape),
        cos_x[:, :half_x].reshape(shape_x),
        sin_x[:, :half_x].reshape(shape_x),
        False,
    )
    flat_shape = (fields, row_count, 1, width_x * width_z * block_y)
    fourth_real, fourth_imag = (
        lax.all_to_all(
            third_real.reshape(flat_shape), "row", split_axis=1, concat_axis=2, tiled=True
        ),
        lax.all_to_all(
            third_imag.reshape(flat_shape), "row", split_axis=1, concat_axis=2, tiled=True
        ),
    )
    deep_shape = (fields, row_count, width_x, width_z, block_y)
    shape_y = (row_count, block_y, full_y)
    return rotate(
        "fparq",
        "pqn",
        "farn",
        fourth_real.reshape(deep_shape),
        fourth_imag.reshape(deep_shape),
        cos_y.reshape(shape_y),
        sin_y.reshape(shape_y),
        False,
    )


def many_physical(real_part, imag_part, tables_all):
    return jnp.concatenate(
        [
            to_physical(real_part[number : number + 1], imag_part[number : number + 1], tables_all)
            for number in range(real_part.shape[0])
        ]
    )


def many_spectral(physical, tables_all, half_x):
    result_list = [
        to_spectral(physical[number : number + 1], tables_all, half_x)
        for number in range(physical.shape[0])
    ]
    return (
        jnp.concatenate([entry[0] for entry in result_list]),
        jnp.concatenate([entry[1] for entry in result_list]),
    )


def body(velocity, accumulator, remesh_flag, remesh_shift, viscosity, shear, clock, step):
    width_x = velocity.shape[2]
    width_z = velocity.shape[3]
    full_y = velocity.shape[4]
    half_x = width_x * lax.axis_size("row")
    NX, NY, NZ = 2 * half_x, full_y, width_z * lax.axis_size("col")
    offset = remesh_flag * remesh_shift
    remeshed = roll_rows(velocity, offset)
    carried = roll_rows(accumulator, offset)
    lattice_x = lax.axis_index("row") * width_x + jnp.arange(width_x, dtype=jnp.int32)
    col_index = lax.axis_index("col") * width_z + jnp.arange(width_z, dtype=jnp.int32)
    lattice_z = signed_index(col_index, NZ)
    lattice_y = signed_index(jnp.arange(full_y, dtype=jnp.int32), NY)
    wave_x = lattice_x.astype(jnp.float32)[:, None, None]
    wave_z = lattice_z.astype(jnp.float32)[None, :, None]
    wave_y = lattice_y.astype(jnp.float32)[None, None, :] - shear[0] * clock[0] * wave_x
    wave_vector = (wave_x, wave_y, wave_z)
    square_wave = wave_x * wave_x + wave_y * wave_y + wave_z * wave_z
    inverse_square = 1.0 / jnp.maximum(square_wave, 1.0)
    dealias_mask = (
        (3 * lattice_x < NX)[:, None, None]
        & (3 * jnp.abs(lattice_z) < NZ)[None, :, None]
        & (3 * jnp.abs(lattice_y) < NY)[None, None, :]
    ).astype(jnp.float32)
    shear_rate = shear[0]
    viscous_rate = viscosity[0]
    stress_part = jnp.sum(
        remeshed[0, 0] * remeshed[1, 0] + remeshed[0, 1] * remeshed[1, 1], axis=(1, 2)
    )
    energy = jnp.sum(remeshed * remeshed, axis=(0, 1))
    dissipation_part = jnp.sum(square_wave * energy, axis=(1, 2))
    stress_total, dissipation_total = lax.psum((stress_part, dissipation_part), "col")
    solen_real, solen_imag = project(remeshed[:, 0], remeshed[:, 1], wave_vector, inverse_square)
    smooth_real = dealias_mask * solen_real
    smooth_imag = dealias_mask * solen_imag
    tables_all = (dft_tables(NY), dft_tables(NX), dft_tables(NZ))
    vort_real = -cross_product(wave_vector, smooth_imag)
    vort_imag = cross_product(wave_vector, smooth_real)
    both_real = jnp.concatenate([smooth_real, vort_real])
    both_imag = jnp.concatenate([smooth_imag, vort_imag])
    physical = many_physical(both_real, both_imag, tables_all)
    lamb_grid = cross_product(physical[:3], physical[3:])
    modes_real, modes_imag = many_spectral(lamb_grid, tables_all, half_x)
    hat_real = dealias_mask * modes_real
    hat_imag = dealias_mask * modes_imag
    proj_real, proj_imag = project(hat_real, hat_imag, wave_vector, inverse_square)
    coupling = 2.0 * shear_rate * wave_x * inverse_square

    def tendency(projected, state):
        term_list = [
            projected[number]
            + coupling * wave_vector[number] * state[1]
            - viscous_rate * square_wave * state[number]
            for number in range(3)
        ]
        term_list[0] = term_list[0] - shear_rate * state[1]
        return jnp.stack(term_list)

    tendencies = jnp.stack(
        [tendency(proj_real, remeshed[:, 0]), tendency(proj_imag, remeshed[:, 1])], axis=1
    )
    new_accumulator = -5.0 / 9.0 * carried + step[0] * tendencies
    new_velocity = remeshed + 15.0 / 16.0 * new_accumulator
    stress = stress_total / (NY * NZ)
    dissipation = 2.0 * viscous_rate * dissipation_total / (NY * NZ)
    return (new_velocity, new_accumulator, jnp.stack([stress, dissipation]))


def angle(rows, cols, n):
    product = np.outer(rows, cols) % n
    return np.cos(2 * np.pi * product / n) / math.sqrt(n), np.sin(2 * np.pi * product / n) / math.sqrt(n)


def halves(table):
    table = np.asarray(table, np.float32)
    high = table.astype(jnp.bfloat16)
    low = (table - high.astype(np.float32)).astype(jnp.bfloat16)
    return jnp.asarray(high), jnp.asarray(low)


def split(x):
    high = x.astype(BF16)
    return high, (x - high.astype(F32)).astype(BF16)


def dot(a, b, dims):
    return lax.dot_general(a, b, (dims, ((), ())), preferred_element_type=F32)


class Sizes:
    def __init__(self, rows, cols, width_x, width_z, full_y):
        self.rows, self.cols = rows, cols
        self.width_x, self.width_z = width_x, width_z
        self.half_x = width_x * rows
        self.full_x = 2 * self.half_x
        self.full_z = width_z * cols
        self.full_y = full_y
        self.block_y = full_y // (rows * cols)
        live = (self.full_x - 1) // 3 + 1
        self.live_x = -(-live // 8) * 8
        self.lanes = 2 * width_z

    def fits(self):
        return (
            self.block_y == 8
            and self.lanes == 128
            and self.full_y % 128 == 0
            and self.full_z % 128 == 0
            and self.full_x % 128 == 0
            and self.width_x % 2 == 0
            and self.rows & (self.rows - 1) == 0
            and self.cols & (self.cols - 1) == 0
        )


def constant_tables(s):
    c, n = angle(np.arange(s.full_y), np.arange(s.full_y), s.full_y)
    y_back = np.concatenate([c, -n], axis=1)
    y_fore = np.concatenate([c, n], axis=1)
    live = np.arange(s.live_x)
    weight = np.where(live == 0, 1.0, 2.0) * (3 * live < s.full_x)
    c, n = angle(np.arange(s.full_x), live, s.full_x)
    x_back = np.concatenate([c * weight, -n * weight], axis=1)
    x_fore = np.concatenate([c.T, -n.T], axis=0)
    c, n = angle(np.arange(s.full_z), np.arange(s.full_z), s.full_z)
    c3, n3 = c.reshape(s.cols, s.width_z, s.full_z), n.reshape(s.cols, s.width_z, s.full_z)
    z_back = np.concatenate(
        [np.concatenate([c3, n3], axis=2), np.concatenate([-n3, c3], axis=2)], axis=1
    )
    ct, nt = c3.transpose(0, 2, 1), n3.transpose(0, 2, 1)
    z_fore = np.concatenate(
        [np.concatenate([ct, -nt], axis=2), np.concatenate([nt, ct], axis=2)], axis=1
    )
    return [halves(t) for t in (y_back, y_fore, x_back, x_fore, z_back, z_fore)]


def whole(shape):
    return pl.BlockSpec(shape, lambda *_: (0,) * len(shape))


def waves(s, kx, col, shear_clock):
    plane = (s.width_z, s.full_y)
    iz = lax.broadcasted_iota(jnp.int32, plane, 0) + col * s.width_z
    iz = jnp.where(2 * iz < s.full_z, iz, iz - s.full_z)
    iy = lax.broadcasted_iota(jnp.int32, plane, 1)
    iy = jnp.where(2 * iy < s.full_y, iy, iy - s.full_y)
    k0 = kx.astype(F32)
    k1 = iy.astype(F32) - shear_clock * k0
    k2 = iz.astype(F32)
    ksq = k0 * k0 + k1 * k1 + k2 * k2
    inverse = 1.0 / jnp.maximum(ksq, 1.0)
    inside = (3 * jnp.abs(iz) < s.full_z) & (3 * jnp.abs(iy) < s.full_y) & (3 * kx < s.full_x)
    return k0, k1, k2, ksq, inverse, inside.astype(F32)


def rolled(s, ref, j, amount):
    flat = jnp.concatenate([ref[c, p, j] for c in range(3) for p in range(2)], axis=0)
    flat = pltpu.roll(flat, lax.rem(s.full_y - amount, s.full_y), 1)
    w = s.width_z
    return [[flat[(2 * c + p) * w : (2 * c + p + 1) * w] for p in range(2)] for c in range(3)]


def head_kernel(s, ints, floats, vel, yh, yl, *outs):
    fields, sums = outs[:3], outs[3]
    row, col = ints[0], ints[1]
    step = pl.program_id(0)
    right = [[], [], []]
    for j in range(2):
        local = 2 * step + j
        kx = row * s.width_x + local
        v = rolled(s, vel, j, ints[2 + local])
        k0, k1, k2, ksq, inverse, mask = waves(s, kx, col, floats[0])
        stress = v[0][0] * v[1][0] + v[0][1] * v[1][1]
        energy = sum(v[c][p] * v[c][p] for c in range(3) for p in range(2))
        fold = lambda a: jnp.sum(a.reshape(s.width_z // 8, 8, s.full_y), axis=0)
        sums[j, 0] = fold(stress)
        sums[j, 1] = fold(ksq * energy)
        along = [(k0 * v[0][p] + k1 * v[1][p] + k2 * v[2][p]) * inverse for p in range(2)]
        for c, k in enumerate((k0, k1, k2)):
            (rh, rl), (ih, il) = [split(mask * (v[c][p] - k * along[p])) for p in range(2)]
            right[c].append(jnp.concatenate([rh, ih, rl, il, rh, ih], axis=1))
            right[c].append(jnp.concatenate([ih, -rh, il, -rl, ih, -rh], axis=1))
    left = jnp.concatenate([yh[...], yh[...], yl[...]], axis=1)
    for c in range(3):
        out = dot(left, jnp.concatenate(right[c], axis=0), ((1,), (1,)))
        for r in range(s.rows):
            for q in range(s.cols):
                at = (r * s.cols + q) * 8
                for j in range(2):
                    fields[c][r, q ^ col, j] = out[at : at + 8, j * 128 : (j + 1) * 128]


def head(s, ints, floats, velocity, table):
    y2 = (s.full_y, 2 * s.full_y)
    piece = (s.rows, s.cols, s.width_x, 8, s.lanes)
    return pl.pallas_call(
        functools.partial(head_kernel, s),
        grid=(s.width_x // 2,),
        in_specs=[
            pl.BlockSpec(memory_space=pltpu.SMEM),
            pl.BlockSpec(memory_space=pltpu.SMEM),
            pl.BlockSpec((3, 2, 2, s.width_z, s.full_y), lambda i: (0, 0, i, 0, 0)),
            whole(y2),
            whole(y2),
        ],
        out_specs=[pl.BlockSpec((s.rows, s.cols, 2, 8, s.lanes), lambda i: (0, 0, i, 0, 0))] * 3
        + [pl.BlockSpec((2, 2, 8, s.full_y), lambda i: (i, 0, 0, 0))],
        out_shape=[jax.ShapeDtypeStruct(piece, F32)] * 3
        + [jax.ShapeDtypeStruct((s.width_x, 2, 8, s.full_y), F32)],
        compiler_params=pltpu.CompilerParams(vmem_limit_bytes=VMEM_LIMIT),
        name="head",
    )(ints, floats, velocity, *table)


def grid_kernel(s, ints, *refs):
    pieces, (zh, zl, xh, xl, out, mid) = refs[: s.cols], refs[s.cols :]
    col = ints[1]
    rows = s.live_x * 8
    step = rows // 4
    zt = jnp.concatenate(
        [zh[q ^ col] for q in range(s.cols)] * 2 + [zl[q ^ col] for q in range(s.cols)], axis=0
    )

    def along_z(i, carry):
        at = pl.multiple_of(i * (step // 8), step // 8)
        parts = [split(p[pl.ds(at, step // 8)].reshape(step, s.lanes)) for p in pieces]
        highs, lows = [h for h, _ in parts], [l for _, l in parts]
        left = jnp.concatenate(highs + lows + highs, axis=1)
        full = dot(left, zt, ((1,), (0,)))
        for t in range(2 * s.full_z // 128):
            mid[t, pl.ds(pl.multiple_of(i * step, step), step)] = full[:, t * 128 : (t + 1) * 128]
        return carry

    lax.fori_loop(0, 4, along_z, 0)
    xt = jnp.concatenate([xh[...], xh[...], xl[...]], axis=1)

    def along_x(y, carry):
        tiles = [mid[t, pl.ds(y, s.live_x, stride=8)] for t in range(2 * s.full_z // 128)]
        half = s.full_z // 128
        both = [jnp.concatenate(tiles[:half], axis=1), jnp.concatenate(tiles[half:], axis=1)]
        high, low = split(jnp.concatenate(both, axis=0))
        out[y] = dot(xt, jnp.concatenate([high, low, high], axis=0), ((1,), (0,)))
        return carry

    lax.fori_loop(0, 8, along_x, 0)


def to_grid(s, ints, pieces, z_table, x_table):
    rows = s.live_x * 8
    return pl.pallas_call(
        functools.partial(grid_kernel, s),
        in_specs=[pl.BlockSpec(memory_space=pltpu.SMEM)]
        + [pl.BlockSpec(memory_space=pltpu.VMEM)] * (s.cols + 4),
        out_specs=pl.BlockSpec(memory_space=pltpu.VMEM),
        out_shape=jax.ShapeDtypeStruct((8, s.full_x, s.full_z), F32),
        scratch_shapes=[pltpu.VMEM((2 * s.full_z // 128, rows, 128), F32)],
        compiler_params=pltpu.CompilerParams(vmem_limit_bytes=VMEM_LIMIT),
        name="to_grid",
    )(ints, *pieces, *z_table, *x_table)


def turn(s, rows, base, kz):
    k0 = ((lax.broadcasted_iota(jnp.int32, (rows, s.lanes), 0) + base) // 8).astype(F32)
    square = k0 * k0 + kz * kz
    scale = lax.rsqrt(jnp.maximum(square, 1.0))
    return jnp.where(square > 0, k0 * scale, 1.0), kz * scale


def back_kernel(s, which, ints, *refs):
    given, _, made = BACK[which]
    u, refs = refs[:given], refs[given:]
    saved, refs = (refs[: s.cols], refs[s.cols :]) if which == 2 else (None, refs)
    (xh, xl, zh, zl), refs = refs[:4], refs[4:]
    outs, mids = refs[: made * s.cols], refs[made * s.cols :]
    col = ints[1]
    xt = jnp.concatenate([xh[...], xh[...], xl[...]], axis=1)

    def along_x(y, carry):
        w = [ref[y] for ref in u]
        if which == 0:
            terms = [w[0] * w[0] - w[1] * w[1], w[0] * w[1]]
        elif which == 1:
            terms = [w[0] * w[1], w[1] * w[2]]
        else:
            terms = [w[0] * w[0] - w[1] * w[1]]
        for mid, term in zip(mids, terms):
            high, low = split(term)
            out = dot(xt, jnp.concatenate([high, low, high], axis=0), ((1,), (0,)))
            half = s.full_z // 128
            for t in range(2 * half):
                p, at = t // half, (t % half) * 128
                tile = out[p * s.live_x : (p + 1) * s.live_x, at : at + 128]
                mid[t, pl.ds(y, s.live_x, stride=8)] = tile
        return carry

    lax.fori_loop(0, 8, along_x, 0)
    rows = s.live_x * 8
    step = rows // 4
    zt = [jnp.concatenate([zh[q ^ col], zh[q ^ col], zl[q ^ col]], axis=0) for q in range(s.cols)]
    zt = jnp.concatenate(zt, axis=1)

    def along_z(i, carry):
        at = pl.multiple_of(i * step, step)
        done = []
        for mid in mids:
            high, low = split(
                jnp.concatenate([mid[t, pl.ds(at, step)] for t in range(2 * s.full_z // 128)], axis=1)
            )
            done.append(dot(jnp.concatenate([high, low, high], axis=1), zt, ((1,), (0,))))
        here = pl.ds(pl.multiple_of(i * (step // 8), step // 8), step // 8)
        shape = (step // 8, 8, s.lanes)
        for q in range(s.cols):
            part = [d[:, q * s.lanes : (q + 1) * s.lanes] for d in done]
            if which == 2:
                outs[q][here] = part[0].reshape(shape) - saved[q][here]
                continue
            lane = lax.broadcasted_iota(jnp.int32, (step, s.lanes), 1)
            iz = lax.rem(lane, s.width_z) + (q ^ col) * s.width_z
            kz = jnp.where(2 * iz < s.full_z, iz, iz - s.full_z).astype(F32)
            cosine, sine = turn(s, step, i * step, kz)
            if which == 0:
                first = cosine * sine * part[0] + (sine * sine - cosine * cosine) * part[1]
                second = cosine * (cosine * part[0] + 2.0 * sine * part[1])
            else:
                first = sine * part[0] - cosine * part[1]
                second = cosine * part[0] + sine * part[1]
            outs[q][here] = first.reshape(shape)
            outs[s.cols + q][here] = second.reshape(shape)
        return carry

    lax.fori_loop(0, 4, along_z, 0)


BACK = ((2, 2, 2), (3, 2, 2), (2, 1, 1))


def products(s, which, ints, fields, x_table, z_table):
    rows = s.live_x * 8
    _, number, made = BACK[which]
    piece = jax.ShapeDtypeStruct((s.live_x, 8, s.lanes), F32)
    out = pl.pallas_call(
        functools.partial(back_kernel, s, which),
        in_specs=[pl.BlockSpec(memory_space=pltpu.SMEM)]
        + [pl.BlockSpec(memory_space=pltpu.VMEM)] * (len(fields) + 4),
        out_specs=[pl.BlockSpec(memory_space=pltpu.VMEM)] * (made * s.cols),
        out_shape=[piece] * (made * s.cols),
        scratch_shapes=[pltpu.VMEM((2 * s.full_z // 128, rows, 128), F32)] * number,
        compiler_params=pltpu.CompilerParams(vmem_limit_bytes=VMEM_LIMIT),
    )(ints, *fields, *x_table, *z_table)
    return [out[i * s.cols : (i + 1) * s.cols] for i in range(made)]


def tail_kernel(s, ints, floats, vel, acc, fa, fb, fc, ff, yh, yl, new_vel, new_acc):
    row, col = ints[0], ints[1]
    local = pl.program_id(0)
    kx = row * s.width_x + local
    amount = ints[2 + local]
    right = jnp.concatenate([yh[...], yh[...], yl[...]], axis=0)
    modes = []
    for ref in (fa, fb, fc, ff):
        tiles = [ref[r, q ^ col, 0] for r in range(s.rows) for q in range(s.cols)]
        high, low = split(jnp.concatenate(tiles, axis=0).T)
        both = dot(jnp.concatenate([high, low, high], axis=1), right, ((1,), (0,)))
        w, n = s.width_z, s.full_y
        modes.append((both[:w, :n] + both[w:, n:], both[w:, :n] - both[:w, n:]))
    k0, k1, k2, ksq, inverse, mask = waves(s, kx, col, floats[0])
    flat = k0 * k0 + k2 * k2
    scale = lax.rsqrt(jnp.maximum(flat, 1.0))
    cosine, sine = jnp.where(flat > 0, k0 * scale, 1.0), k2 * scale
    kh = flat * scale
    lean = (flat - k1 * k1) * inverse
    cross = kh * k1 * inverse
    v = rolled(s, vel, 0, amount)
    old = rolled(s, acc, 0, amount)
    shear, viscosity, dt = floats[1], floats[2], floats[3]
    coupling = (2.0 * shear) * k0 * inverse
    for p in range(2):
        a, b, c, f = [m[1 - p] for m in modes]
        sign = mask if p == 0 else -mask
        qt = (kh * a + k1 * b) * sign
        qe = (lean * c + cross * f) * sign
        slope = qe * k1
        nonlinear = (qt * sine - slope * cosine, qe * kh, -(qt * cosine) - slope * sine)
        drive = coupling * v[1][p]
        for c3, k in enumerate((k0, k1, k2)):
            rate = nonlinear[c3] + k * drive - (viscosity * ksq) * v[c3][p]
            if c3 == 0:
                rate = rate - shear * v[1][p]
            fresh = (-5.0 / 9.0) * old[c3][p] + dt * rate
            new_acc[c3, p, 0] = fresh
            new_vel[c3, p, 0] = v[c3][p] + (15.0 / 16.0) * fresh


def tail(s, ints, floats, velocity, accumulator, fields, table):
    plane = pl.BlockSpec((3, 2, 1, s.width_z, s.full_y), lambda i: (0, 0, i, 0, 0))
    piece = pl.BlockSpec((s.rows, s.cols, 1, 8, s.lanes), lambda i: (0, 0, i, 0, 0))
    y2 = (s.full_y, 2 * s.full_y)
    shape = jax.ShapeDtypeStruct(velocity.shape, F32)
    return pl.pallas_call(
        functools.partial(tail_kernel, s),
        grid=(s.width_x,),
        in_specs=[pl.BlockSpec(memory_space=pltpu.SMEM)] * 2 + [plane] * 2 + [piece] * 4 + [whole(y2)] * 2,
        out_specs=[plane] * 2,
        out_shape=[shape] * 2,
        compiler_params=pltpu.CompilerParams(vmem_limit_bytes=VMEM_LIMIT),
        name="tail",
    )(ints, floats, velocity, accumulator, *fields, *table)


def col_exchange(s, pieces):
    out = [pieces[0]]
    for q in range(1, s.cols):
        out.append(lax.ppermute(pieces[q], "col", [(i, i ^ q) for i in range(s.cols)]))
    return out


def row_exchange(field):
    return lax.all_to_all(field, "row", 0, 0, tiled=True)


def forward_field(s, field):
    got = row_exchange(field)
    pieces = [
        got[:, q].reshape(s.half_x, 8, s.lanes)[: s.live_x] for q in range(s.cols)
    ]
    return col_exchange(s, pieces)


def backward_field(s, pieces):
    got = col_exchange(s, pieces)
    spare = ((0, s.half_x - s.live_x), (0, 0), (0, 0))
    both = jnp.stack(
        [jnp.pad(p, spare).reshape(s.rows, s.width_x, 8, s.lanes) for p in got], axis=1
    )
    return row_exchange(both)


def tiled_body(s, velocity, accumulator, remesh_flag, remesh_shift, viscosity, shear, clock, step):
    y_back, y_fore, x_back, x_fore, z_back, z_fore = constant_tables(s)
    place = jnp.stack([lax.axis_index("row"), lax.axis_index("col")]).astype(jnp.int32)
    ints = jnp.concatenate([place, remesh_flag * remesh_shift])
    floats = jnp.concatenate([shear * clock, shear, viscosity, step])
    v0, v1, v2, sums = head(s, ints, floats, velocity, y_back)

    def up(field):
        return to_grid(s, ints, forward_field(s, field), z_back, x_back)

    u0, u2, u1 = up(v0), up(v2), up(v1)
    a, kept = products(s, 0, ints, [u0, u2], x_fore, z_fore)
    b, c = products(s, 1, ints, [u0, u1, u2], x_fore, z_fore)
    (f,) = products(s, 2, ints, [u1, u2, *kept], x_fore, z_fore)
    a, b, c, f = [backward_field(s, q) for q in (a, b, c, f)]
    totals = lax.psum(jnp.sum(sums, axis=(2, 3)), "col") / (s.full_y * s.full_z)
    spectra = jnp.stack([totals[:, 0], 2.0 * viscosity[0] * totals[:, 1]])
    new_velocity, new_accumulator = tail(
        s, ints, floats, velocity, accumulator, (a, b, c, f), y_fore
    )
    return new_velocity, new_accumulator, spectra


def solution(mesh):
    in_specs = (
        P(None, None, "row", "col", None),
        P(None, None, "row", "col", None),
        P("row"),
        P("row"),
        P(),
        P(),
        P(),
        P(),
    )
    out_specs = (
        P(None, None, "row", "col", None),
        P(None, None, "row", "col", None),
        P(None, "row"),
    )
    rows, cols = mesh.shape["row"], mesh.shape["col"]

    def local(velocity, *rest):
        s = Sizes(rows, cols, velocity.shape[2], velocity.shape[3], velocity.shape[4])
        run = functools.partial(tiled_body, s) if s.fits() else body
        return run(velocity, *rest)

    return jax.shard_map(local, mesh=mesh, in_specs=in_specs, out_specs=out_specs, check_vma=False)
```

```python
import functools
import math

import jax
import jax.numpy as jnp
import numpy as np
from jax import lax
from jax.experimental import pallas as pl
from jax.experimental.pallas import tpu as pltpu
from jax.sharding import PartitionSpec as P


F32 = jnp.float32
BF16 = jnp.bfloat16
VMEM_LIMIT = 56 * 1024 * 1024


def signed_index(positions, period):
    return jnp.where(2 * positions < period, positions, positions - period)


def roll_rows(field, amounts):

    def shift_row(row_data, amount_one):
        return jnp.roll(row_data, -amount_one, axis=-1)

    return jax.vmap(shift_row, in_axes=(2, 0), out_axes=2)(field, amounts)


def dft_tables(period):
    positions = jnp.arange(period, dtype=jnp.int32)
    product = positions[:, None] * positions[None, :] % period
    angles = product.astype(jnp.float32) * (2.0 * math.pi / period)
    factor = 1.0 / math.sqrt(period)
    return (jnp.cos(angles) * factor, jnp.sin(angles) * factor)


def product_high(formula, first_arg, second_arg):
    return jnp.einsum(formula, first_arg, second_arg, precision=lax.Precision.HIGHEST)


def rotate(left_side, right_side, output, real_part, imag_part, cosine_table, sine_table, backward):
    stacked = jnp.stack([real_part, imag_part])
    if backward:
        block_table = jnp.stack(
            [jnp.stack([cosine_table, sine_table]), jnp.stack([-sine_table, cosine_table])]
        )
    else:
        block_table = jnp.stack(
            [jnp.stack([cosine_table, -sine_table]), jnp.stack([sine_table, cosine_table])]
        )
    result = product_high(
        "s" + left_side + ",st" + right_side + "->t" + output, stacked, block_table
    )
    return (result[0], result[1])


def project(real_part, imag_part, wave_vector, inverse_square):
    along_real = (
        wave_vector[0] * real_part[0]
        + wave_vector[1] * real_part[1]
        + wave_vector[2] * real_part[2]
    ) * inverse_square
    along_imag = (
        wave_vector[0] * imag_part[0]
        + wave_vector[1] * imag_part[1]
        + wave_vector[2] * imag_part[2]
    ) * inverse_square
    return (
        jnp.stack([real_part[number] - wave_vector[number] * along_real for number in range(3)]),
        jnp.stack([imag_part[number] - wave_vector[number] * along_imag for number in range(3)]),
    )


def cross_product(first_one, second_one):
    return jnp.stack(
        [
            first_one[1] * second_one[2] - first_one[2] * second_one[1],
            first_one[2] * second_one[0] - first_one[0] * second_one[2],
            first_one[0] * second_one[1] - first_one[1] * second_one[0],
        ]
    )


def to_physical(real_part, imag_part, tables_all):
    (cos_y, sin_y), (cos_x, sin_x), (cos_z, sin_z) = tables_all
    row_count = lax.axis_size("row")
    col_count = lax.axis_size("col")
    fields, width_x, width_z, full_y = real_part.shape
    block_y = full_y // row_count
    half_x = width_x * row_count
    full_x = cos_x.shape[0]
    block_x = full_x // col_count
    full_z = width_z * col_count
    shape_y = (full_y, row_count, block_y)
    first_real, first_imag = rotate(
        "fabc",
        "cpq",
        "fpabq",
        real_part,
        imag_part,
        cos_y.reshape(shape_y),
        sin_y.reshape(shape_y),
        True,
    )
    flat_shape = (fields, row_count, width_x, width_z * block_y)
    second_real, second_imag = (
        lax.all_to_all(
            first_real.reshape(flat_shape), "row", split_axis=1, concat_axis=2, tiled=True
        ),
        lax.all_to_all(
            first_imag.reshape(flat_shape), "row", split_axis=1, concat_axis=2, tiled=True
        ),
    )
    deep_shape = (fields, half_x, width_z, block_y)
    weights = jnp.where(jnp.arange(half_x) == 0, 1.0, 2.0).astype(jnp.float32)[:, None]
    shape_x = (half_x, col_count, block_x)
    cos_half = (weights * cos_x[:half_x]).reshape(shape_x)
    sin_half = (weights * sin_x[:half_x]).reshape(shape_x)
    third_real, third_imag = rotate(
        "fkzy",
        "kpq",
        "fpzyq",
        second_real.reshape(deep_shape),
        second_imag.reshape(deep_shape),
        cos_half,
        sin_half,
        True,
    )
    flat_shape = (fields, col_count, 1, width_z * block_y * block_x)
    fourth_real, fourth_imag = (
        lax.all_to_all(
            third_real.reshape(flat_shape), "col", split_axis=1, concat_axis=2, tiled=True
        ),
        lax.all_to_all(
            third_imag.reshape(flat_shape), "col", split_axis=1, concat_axis=2, tiled=True
        ),
    )
    deep_shape = (fields, col_count, width_z, block_y, block_x)
    shape_z = (col_count, width_z, full_z)
    stacked = jnp.stack([fourth_real.reshape(deep_shape), fourth_imag.reshape(deep_shape)])
    z_table = jnp.stack([cos_z.reshape(shape_z), -sin_z.reshape(shape_z)])
    return product_high("sfpkyq,spkn->fyqn", stacked, z_table)


def to_spectral(physical, tables_all, half_x):
    (cos_y, sin_y), (cos_x, sin_x), (cos_z, sin_z) = tables_all
    row_count = lax.axis_size("row")
    col_count = lax.axis_size("col")
    fields, block_y, block_x, full_z = physical.shape
    width_z = full_z // col_count
    width_x = half_x // row_count
    full_y = block_y * row_count
    shape_z = (full_z, col_count, width_z)
    z_table = jnp.stack([cos_z.reshape(shape_z), -sin_z.reshape(shape_z)])
    first_both = product_high("fyqn,tnpk->tfpkyq", physical, z_table)
    first_real, first_imag = (first_both[0], first_both[1])
    flat_shape = (fields, col_count, 1, width_z * block_y * block_x)
    second_real, second_imag = (
        lax.all_to_all(
            first_real.reshape(flat_shape), "col", split_axis=1, concat_axis=2, tiled=True
        ),
        lax.all_to_all(
            first_imag.reshape(flat_shape), "col", split_axis=1, concat_axis=2, tiled=True
        ),
    )
    deep_shape = (fields, col_count, width_z, block_y, block_x)
    shape_x = (col_count, block_x, row_count, width_x)
    third_real, third_imag = rotate(
        "fpkyq",
        "pqmr",
        "fmrky",
        second_real.reshape(deep_shape),
        second_imag.reshape(deep_shape),
        cos_x[:, :half_x].reshape(shape_x),
        sin_x[:, :half_x].reshape(shape_x),
        False,
    )
    flat_shape = (fields, row_count, 1, width_x * width_z * block_y)
    fourth_real, fourth_imag = (
        lax.all_to_all(
            third_real.reshape(flat_shape), "row", split_axis=1, concat_axis=2, tiled=True
        ),
        lax.all_to_all(
            third_imag.reshape(flat_shape), "row", split_axis=1, concat_axis=2, tiled=True
        ),
    )
    deep_shape = (fields, row_count, width_x, width_z, block_y)
    shape_y = (row_count, block_y, full_y)
    return rotate(
        "fparq",
        "pqn",
        "farn",
        fourth_real.reshape(deep_shape),
        fourth_imag.reshape(deep_shape),
        cos_y.reshape(shape_y),
        sin_y.reshape(shape_y),
        False,
    )


def many_physical(real_part, imag_part, tables_all):
    return jnp.concatenate(
        [
            to_physical(real_part[number : number + 1], imag_part[number : number + 1], tables_all)
            for number in range(real_part.shape[0])
        ]
    )


def many_spectral(physical, tables_all, half_x):
    result_list = [
        to_spectral(physical[number : number + 1], tables_all, half_x)
        for number in range(physical.shape[0])
    ]
    return (
        jnp.concatenate([entry[0] for entry in result_list]),
        jnp.concatenate([entry[1] for entry in result_list]),
    )


def body(velocity, accumulator, remesh_flag, remesh_shift, viscosity, shear, clock, step):
    width_x = velocity.shape[2]
    width_z = velocity.shape[3]
    full_y = velocity.shape[4]
    half_x = width_x * lax.axis_size("row")
    NX, NY, NZ = 2 * half_x, full_y, width_z * lax.axis_size("col")
    offset = remesh_flag * remesh_shift
    remeshed = roll_rows(velocity, offset)
    carried = roll_rows(accumulator, offset)
    lattice_x = lax.axis_index("row") * width_x + jnp.arange(width_x, dtype=jnp.int32)
    col_index = lax.axis_index("col") * width_z + jnp.arange(width_z, dtype=jnp.int32)
    lattice_z = signed_index(col_index, NZ)
    lattice_y = signed_index(jnp.arange(full_y, dtype=jnp.int32), NY)
    wave_x = lattice_x.astype(jnp.float32)[:, None, None]
    wave_z = lattice_z.astype(jnp.float32)[None, :, None]
    wave_y = lattice_y.astype(jnp.float32)[None, None, :] - shear[0] * clock[0] * wave_x
    wave_vector = (wave_x, wave_y, wave_z)
    square_wave = wave_x * wave_x + wave_y * wave_y + wave_z * wave_z
    inverse_square = 1.0 / jnp.maximum(square_wave, 1.0)
    dealias_mask = (
        (3 * lattice_x < NX)[:, None, None]
        & (3 * jnp.abs(lattice_z) < NZ)[None, :, None]
        & (3 * jnp.abs(lattice_y) < NY)[None, None, :]
    ).astype(jnp.float32)
    shear_rate = shear[0]
    viscous_rate = viscosity[0]
    stress_part = jnp.sum(
        remeshed[0, 0] * remeshed[1, 0] + remeshed[0, 1] * remeshed[1, 1], axis=(1, 2)
    )
    energy = jnp.sum(remeshed * remeshed, axis=(0, 1))
    dissipation_part = jnp.sum(square_wave * energy, axis=(1, 2))
    stress_total, dissipation_total = lax.psum((stress_part, dissipation_part), "col")
    solen_real, solen_imag = project(remeshed[:, 0], remeshed[:, 1], wave_vector, inverse_square)
    smooth_real = dealias_mask * solen_real
    smooth_imag = dealias_mask * solen_imag
    tables_all = (dft_tables(NY), dft_tables(NX), dft_tables(NZ))
    vort_real = -cross_product(wave_vector, smooth_imag)
    vort_imag = cross_product(wave_vector, smooth_real)
    both_real = jnp.concatenate([smooth_real, vort_real])
    both_imag = jnp.concatenate([smooth_imag, vort_imag])
    physical = many_physical(both_real, both_imag, tables_all)
    lamb_grid = cross_product(physical[:3], physical[3:])
    modes_real, modes_imag = many_spectral(lamb_grid, tables_all, half_x)
    hat_real = dealias_mask * modes_real
    hat_imag = dealias_mask * modes_imag
    proj_real, proj_imag = project(hat_real, hat_imag, wave_vector, inverse_square)
    coupling = 2.0 * shear_rate * wave_x * inverse_square

    def tendency(projected, state):
        term_list = [
            projected[number]
            + coupling * wave_vector[number] * state[1]
            - viscous_rate * square_wave * state[number]
            for number in range(3)
        ]
        term_list[0] = term_list[0] - shear_rate * state[1]
        return jnp.stack(term_list)

    tendencies = jnp.stack(
        [tendency(proj_real, remeshed[:, 0]), tendency(proj_imag, remeshed[:, 1])], axis=1
    )
    new_accumulator = -5.0 / 9.0 * carried + step[0] * tendencies
    new_velocity = remeshed + 15.0 / 16.0 * new_accumulator
    stress = stress_total / (NY * NZ)
    dissipation = 2.0 * viscous_rate * dissipation_total / (NY * NZ)
    return (new_velocity, new_accumulator, jnp.stack([stress, dissipation]))


def angle(rows, cols, n):
    product = np.outer(rows, cols) % n
    return np.cos(2 * np.pi * product / n) / math.sqrt(n), np.sin(2 * np.pi * product / n) / math.sqrt(n)


def halves(table):
    table = np.asarray(table, np.float32)
    high = table.astype(jnp.bfloat16)
    low = (table - high.astype(np.float32)).astype(jnp.bfloat16)
    return high, low


def split(x):
    high = x.astype(BF16)
    return high, (x - high.astype(F32)).astype(BF16)


def dot(a, b, dims):
    return lax.dot_general(a, b, (dims, ((), ())), preferred_element_type=F32)


class Sizes:
    def __init__(self, rows, cols, width_x, width_z, full_y):
        self.rows, self.cols = rows, cols
        self.width_x, self.width_z = width_x, width_z
        self.half_x = width_x * rows
        self.full_x = 2 * self.half_x
        self.full_z = width_z * cols
        self.full_y = full_y
        self.block_y = full_y // (rows * cols)
        live = (self.full_x - 1) // 3 + 1
        self.live_x = -(-live // 8) * 8
        self.lanes = 2 * width_z

    def fits(self):
        return (
            self.block_y == 8
            and self.cols == 4
            and self.lanes == 128
            and self.full_y % 128 == 0
            and self.full_z % 128 == 0
            and self.full_x % 128 == 0
            and self.width_x % 2 == 0
            and self.rows & (self.rows - 1) == 0
            and self.cols & (self.cols - 1) == 0
        )


def constant_tables(s):
    c, n = angle(np.arange(s.full_y), np.arange(s.full_y), s.full_y)
    y_back = np.concatenate([c, -n], axis=1)
    y_fore = np.concatenate([c, n], axis=1)
    live = np.arange(s.live_x)
    weight = np.where(live == 0, 1.0, 2.0) * (3 * live < s.full_x)
    c, n = angle(np.arange(s.full_x), live, s.full_x)
    x_back = np.concatenate([c * weight, -n * weight], axis=1)
    x_fore = np.concatenate([c.T, -n.T], axis=0)
    c, n = angle(np.arange(s.full_z), np.arange(s.full_z), s.full_z)
    c3, n3 = c.reshape(s.cols, s.width_z, s.full_z), n.reshape(s.cols, s.width_z, s.full_z)
    z_back = np.concatenate(
        [np.concatenate([c3, n3], axis=2), np.concatenate([-n3, c3], axis=2)], axis=1
    )
    ct, nt = c3.transpose(0, 2, 1), n3.transpose(0, 2, 1)
    z_fore = np.concatenate(
        [np.concatenate([ct, -nt], axis=2), np.concatenate([nt, ct], axis=2)], axis=1
    )
    left = [np.concatenate(halves(t), axis=0) for t in (y_back, x_back, x_fore)]
    return left + [halves(t) for t in (y_fore, z_back, z_fore)]


def by_left_table(table, rows, high, low, inner):
    out = dot(table[...], high, inner)
    return out[:rows] + (out[rows:] + dot(table[:rows], low, inner))


def by_right_table(data, high, low):
    n = data.shape[0]
    top, rest = split(data)
    out = dot(jnp.concatenate([top, rest], axis=0), high, ((1,), (0,)))
    return out[:n] + (out[n:] + dot(top, low, ((1,), (0,))))


def whole(shape):
    return pl.BlockSpec(shape, lambda *_: (0,) * len(shape))


def waves(s, kx, col, shear_clock):
    plane = (s.width_z, s.full_y)
    iz = lax.broadcasted_iota(jnp.int32, plane, 0) + col * s.width_z
    iz = jnp.where(2 * iz < s.full_z, iz, iz - s.full_z)
    iy = lax.broadcasted_iota(jnp.int32, plane, 1)
    iy = jnp.where(2 * iy < s.full_y, iy, iy - s.full_y)
    k0 = kx.astype(F32)
    k1 = iy.astype(F32) - shear_clock * k0
    k2 = iz.astype(F32)
    ksq = k0 * k0 + k1 * k1 + k2 * k2
    inverse = 1.0 / jnp.maximum(ksq, 1.0)
    inside = (3 * jnp.abs(iz) < s.full_z) & (3 * jnp.abs(iy) < s.full_y) & (3 * kx < s.full_x)
    return k0, k1, k2, ksq, inverse, inside.astype(F32)


def rolled(s, ref, j, amount):
    flat = jnp.concatenate([ref[c, p, j] for c in range(3) for p in range(2)], axis=0)
    flat = pltpu.roll(flat, lax.rem(s.full_y - amount, s.full_y), 1)
    w = s.width_z
    return [[flat[(2 * c + p) * w : (2 * c + p + 1) * w] for p in range(2)] for c in range(3)]


def head_kernel(s, ints, floats, vel, table, *outs):
    fields, sums, made = outs[:-2], outs[-2], outs[-1]
    row, col = ints[0], ints[1]
    step = pl.program_id(0)
    right = [[], [], []]
    for j in range(2):
        local = 2 * step + j
        kx = row * s.width_x + local
        v = rolled(s, vel, j, ints[2 + local])
        k0, k1, k2, ksq, inverse, mask = waves(s, kx, col, floats[0])
        stress = v[0][0] * v[1][0] + v[0][1] * v[1][1]
        energy = sum(v[c][p] * v[c][p] for c in range(3) for p in range(2))
        fold = lambda a: jnp.sum(a.reshape(s.width_z // 8, 8, s.full_y), axis=0)
        sums[j, 0] = fold(stress)
        sums[j, 1] = fold(ksq * energy)
        along = [(k0 * v[0][p] + k1 * v[1][p] + k2 * v[2][p]) * inverse for p in range(2)]
        for c, k in enumerate((k0, k1, k2)):
            (rh, rl), (ih, il) = [split(mask * (v[c][p] - k * along[p])) for p in range(2)]
            right[c].append([jnp.concatenate([rh, ih], axis=1), jnp.concatenate([rl, il], axis=1)])
            right[c].append([jnp.concatenate([ih, -rh], axis=1), jnp.concatenate([il, -rl], axis=1)])
    for c in range(3):
        high, low = [jnp.concatenate([x[i] for x in right[c]], axis=0) for i in range(2)]
        made[...] = by_left_table(table, s.full_y, high, low, ((1,), (1,)))
        for r in range(s.rows):
            for q in range(s.cols):
                at = pl.multiple_of((r * s.cols + (q ^ col)) * 8, 8)
                for j in range(2):
                    tile = made[pl.ds(at, 8), j * 128 : (j + 1) * 128]
                    if c < 2:
                        fields[c][r, q, j] = tile
                    else:
                        fields[c + q][r, j] = tile


def head(s, ints, floats, velocity, table):
    out = pl.pallas_call(
        functools.partial(head_kernel, s),
        grid=(s.width_x // 2,),
        in_specs=[
            pl.BlockSpec(memory_space=pltpu.SMEM),
            pl.BlockSpec(memory_space=pltpu.SMEM),
            pl.BlockSpec((3, 2, 2, s.width_z, s.full_y), lambda i: (0, 0, i, 0, 0)),
            whole(table.shape),
        ],
        out_specs=[pl.BlockSpec((s.rows, s.cols, 2, 8, s.lanes), lambda i: (0, 0, i, 0, 0))] * 2
        + [pl.BlockSpec((s.rows, 2, 8, s.lanes), lambda i: (0, i, 0, 0))] * s.cols
        + [pl.BlockSpec((2, 2, 8, s.full_y), lambda i: (i, 0, 0, 0))],
        out_shape=[jax.ShapeDtypeStruct((s.rows, s.cols, s.width_x, 8, s.lanes), F32)] * 2
        + [jax.ShapeDtypeStruct((s.rows, s.width_x, 8, s.lanes), F32)] * s.cols
        + [jax.ShapeDtypeStruct((s.width_x, 2, 8, s.full_y), F32)],
        scratch_shapes=[pltpu.VMEM((s.full_y, 256), F32)],
        compiler_params=pltpu.CompilerParams(vmem_limit_bytes=VMEM_LIMIT),
        name="head",
    )(ints, floats, velocity, table)
    return out[0], out[1], out[2:-1], out[-1]


def grid_kernel(s, ints, *refs):
    pieces, (zh, zl, x_table, out, mid) = refs[: s.cols], refs[s.cols :]
    col = ints[1]
    rows = s.live_x * 8
    step = rows // 2
    high_z = jnp.concatenate([zh[q ^ col] for q in range(s.cols)], axis=0)
    low_z = jnp.concatenate([zl[q ^ col] for q in range(s.cols)], axis=0)

    def along_z(i, carry):
        at = pl.multiple_of(i * (step // 8), step // 8)
        parts = [p[pl.ds(at, step // 8)].reshape(step, s.lanes) for p in pieces]
        full = by_right_table(jnp.concatenate(parts, axis=1), high_z, low_z)
        for t in range(2 * s.full_z // 128):
            mid[t, pl.ds(pl.multiple_of(i * step, step), step)] = full[:, t * 128 : (t + 1) * 128]
        return carry

    lax.fori_loop(0, 2, along_z, 0)

    def along_x(y, carry):
        tiles = [mid[t, pl.ds(y, s.live_x, stride=8)] for t in range(2 * s.full_z // 128)]
        half = s.full_z // 128
        both = [jnp.concatenate(tiles[:half], axis=1), jnp.concatenate(tiles[half:], axis=1)]
        high, low = split(jnp.concatenate(both, axis=0))
        out[y] = by_left_table(x_table, s.full_x, high, low, ((1,), (0,)))
        return carry

    lax.fori_loop(0, 8, along_x, 0)


def to_grid(s, ints, pieces, z_table, x_table):
    rows = s.live_x * 8
    return pl.pallas_call(
        functools.partial(grid_kernel, s),
        in_specs=[pl.BlockSpec(memory_space=pltpu.SMEM)]
        + [pl.BlockSpec(memory_space=pltpu.VMEM)] * (s.cols + 3),
        out_specs=pl.BlockSpec(memory_space=pltpu.VMEM),
        out_shape=jax.ShapeDtypeStruct((8, s.full_x, s.full_z), F32),
        scratch_shapes=[pltpu.VMEM((2 * s.full_z // 128, rows, 128), F32)],
        compiler_params=pltpu.CompilerParams(vmem_limit_bytes=VMEM_LIMIT),
        name="to_grid",
    )(ints, *pieces, *z_table, x_table)


def turn(s, rows, base, kz):
    k0 = ((lax.broadcasted_iota(jnp.int32, (rows, s.lanes), 0) + base) // 8).astype(F32)
    square = k0 * k0 + kz * kz
    scale = lax.rsqrt(jnp.maximum(square, 1.0))
    return jnp.where(square > 0, k0 * scale, 1.0), kz * scale


def back_kernel(s, which, ints, *refs):
    given, _, made = BACK[which]
    u, refs = refs[:given], refs[given:]
    saved, refs = (refs[: s.cols], refs[s.cols :]) if which == 2 else (None, refs)
    (x_table, zh, zl), refs = refs[:3], refs[3:]
    outs, mids = refs[: made * s.cols], refs[made * s.cols :]
    col = ints[1]

    def along_x(y, carry):
        w = [ref[y] for ref in u]
        if which == 0:
            terms = [w[0] * w[0] - w[1] * w[1], w[0] * w[1]]
        elif which == 1:
            terms = [w[0] * w[1], w[1] * w[2]]
        else:
            terms = [w[0] * w[0] - w[1] * w[1]]
        for mid, term in zip(mids, terms):
            high, low = split(term)
            out = by_left_table(x_table, 2 * s.live_x, high, low, ((1,), (0,)))
            half = s.full_z // 128
            for t in range(2 * half):
                p, at = t // half, (t % half) * 128
                tile = out[p * s.live_x : (p + 1) * s.live_x, at : at + 128]
                mid[t, pl.ds(y, s.live_x, stride=8)] = tile
        return carry

    lax.fori_loop(0, 8, along_x, 0)
    rows = s.live_x * 8
    step = rows // 2
    high_z = jnp.concatenate([zh[q ^ col] for q in range(s.cols)], axis=1)
    low_z = jnp.concatenate([zl[q ^ col] for q in range(s.cols)], axis=1)

    def along_z(i, carry):
        at = pl.multiple_of(i * step, step)
        done = []
        for mid in mids:
            data = [mid[t, pl.ds(at, step)] for t in range(2 * s.full_z // 128)]
            done.append(by_right_table(jnp.concatenate(data, axis=1), high_z, low_z))
        here = pl.ds(pl.multiple_of(i * (step // 8), step // 8), step // 8)
        shape = (step // 8, 8, s.lanes)
        for q in range(s.cols):
            part = [d[:, q * s.lanes : (q + 1) * s.lanes] for d in done]
            if which == 2:
                outs[q][here] = part[0].reshape(shape) - saved[q][here]
                continue
            lane = lax.broadcasted_iota(jnp.int32, (step, s.lanes), 1)
            iz = lax.rem(lane, s.width_z) + (q ^ col) * s.width_z
            kz = jnp.where(2 * iz < s.full_z, iz, iz - s.full_z).astype(F32)
            cosine, sine = turn(s, step, i * step, kz)
            if which == 0:
                first = cosine * sine * part[0] + (sine * sine - cosine * cosine) * part[1]
                second = cosine * (cosine * part[0] + 2.0 * sine * part[1])
            else:
                first = sine * part[0] - cosine * part[1]
                second = cosine * part[0] + sine * part[1]
            outs[q][here] = first.reshape(shape)
            outs[s.cols + q][here] = second.reshape(shape)
        return carry

    lax.fori_loop(0, 2, along_z, 0)


BACK = ((2, 2, 2), (3, 2, 2), (2, 1, 1))


def products(s, which, ints, fields, x_table, z_table):
    rows = s.live_x * 8
    _, number, made = BACK[which]
    piece = jax.ShapeDtypeStruct((s.live_x, 8, s.lanes), F32)
    out = pl.pallas_call(
        functools.partial(back_kernel, s, which),
        in_specs=[pl.BlockSpec(memory_space=pltpu.SMEM)]
        + [pl.BlockSpec(memory_space=pltpu.VMEM)] * (len(fields) + 3),
        out_specs=[pl.BlockSpec(memory_space=pltpu.VMEM)] * (made * s.cols),
        out_shape=[piece] * (made * s.cols),
        scratch_shapes=[pltpu.VMEM((2 * s.full_z // 128, rows, 128), F32)] * number,
        compiler_params=pltpu.CompilerParams(vmem_limit_bytes=VMEM_LIMIT),
    )(ints, *fields, x_table, *z_table)
    return [out[i * s.cols : (i + 1) * s.cols] for i in range(made)]


def frame(s, kx, col, shear_clock):
    k0, k1, k2, ksq, inverse, mask = waves(s, kx, col, shear_clock)
    flat = k0 * k0 + k2 * k2
    scale = lax.rsqrt(jnp.maximum(flat, 1.0))
    cosine, sine = jnp.where(flat > 0, k0 * scale, 1.0), k2 * scale
    return (k0, k1, k2), ksq, inverse, mask, flat, flat * scale, cosine, sine


def modes_of(s, col, refs, yh, yl):
    turned = []
    for ref in refs:
        tiles = [ref[r, q ^ col, 0] for r in range(s.rows) for q in range(s.cols)]
        turned.append(jnp.concatenate(tiles, axis=0).T)
    every = by_right_table(jnp.concatenate(turned, axis=0), yh[...], yl[...])
    modes = []
    w, n = s.width_z, s.full_y
    for i in range(len(refs)):
        both = every[i * s.lanes : (i + 1) * s.lanes]
        modes.append((both[:w, :n] + both[w:, n:], both[w:, :n] - both[:w, n:]))
    return modes


def early_kernel(s, ints, floats, vel, acc, fa, fb, yh, yl, new_vel, new_acc):
    row, col = ints[0], ints[1]
    local = pl.program_id(0)
    kx, amount = row * s.width_x + local, ints[2 + local]
    modes = modes_of(s, col, (fa, fb), yh, yl)
    k, ksq, inverse, mask, _, kh, cosine, sine = frame(s, kx, col, floats[0])
    v = rolled(s, vel, 0, amount)
    old = rolled(s, acc, 0, amount)
    shear, viscosity, dt = floats[1], floats[2], floats[3]
    coupling = (2.0 * shear) * k[0] * inverse
    for p in range(2):
        a, b = [m[1 - p] for m in modes]
        qt = (kh * a + k[1] * b) * (mask if p == 0 else -mask)
        nonlinear = (qt * sine, None, -(qt * cosine))
        drive = coupling * v[1][p]
        for c3 in range(3):
            rate = k[c3] * drive - (viscosity * ksq) * v[c3][p]
            if c3 != 1:
                rate = rate + nonlinear[c3]
            if c3 == 0:
                rate = rate - shear * v[1][p]
            fresh = (-5.0 / 9.0) * old[c3][p] + dt * rate
            new_acc[c3, p, 0] = fresh
            new_vel[c3, p, 0] = v[c3][p] + (15.0 / 16.0) * fresh


def late_kernel(s, ints, floats, vel, acc, fc, ff, yh, yl, new_vel, new_acc):
    row, col = ints[0], ints[1]
    kx = row * s.width_x + pl.program_id(0)
    modes = modes_of(s, col, (fc, ff), yh, yl)
    k, _, inverse, mask, flat, kh, cosine, sine = frame(s, kx, col, floats[0])
    dt = floats[3] * mask
    lean = dt * (flat - k[1] * k[1]) * inverse
    cross = dt * kh * k[1] * inverse
    for p in range(2):
        c, f = [m[1 - p] for m in modes]
        qe = lean * c + cross * f
        if p == 1:
            qe = -qe
        slope = qe * k[1]
        for c3, add in enumerate((-(slope * cosine), qe * kh, -(slope * sine))):
            new_acc[c3, p, 0] = acc[c3, p, 0] + add
            new_vel[c3, p, 0] = vel[c3, p, 0] + (15.0 / 16.0) * add


def update(s, kernel, ints, floats, velocity, accumulator, fields, table, alias):
    plane = pl.BlockSpec((3, 2, 1, s.width_z, s.full_y), lambda i: (0, 0, i, 0, 0))
    piece = pl.BlockSpec((s.rows, s.cols, 1, 8, s.lanes), lambda i: (0, 0, i, 0, 0))
    y2 = (s.full_y, 2 * s.full_y)
    shape = jax.ShapeDtypeStruct(velocity.shape, F32)
    return pl.pallas_call(
        functools.partial(kernel, s),
        grid=(s.width_x,),
        in_specs=[pl.BlockSpec(memory_space=pltpu.SMEM)] * 2
        + [plane] * 2
        + [piece] * 2
        + [whole(y2)] * 2,
        out_specs=[plane] * 2,
        out_shape=[shape] * 2,
        input_output_aliases=alias,
        compiler_params=pltpu.CompilerParams(vmem_limit_bytes=VMEM_LIMIT),
    )(ints, floats, velocity, accumulator, *fields, *table)


def col_exchange(s, pieces):
    out = [pieces[0]]
    for q in range(1, s.cols):
        out.append(lax.ppermute(pieces[q], "col", [(i, i ^ q) for i in range(s.cols)]))
    return out


def row_exchange(field):
    return lax.all_to_all(field, "row", 0, 0, tiled=True)


def of_cols(s, got):
    return [got[:, q].reshape(s.half_x, 8, s.lanes)[: s.live_x] for q in range(s.cols)]


def spread_kernel(s, *refs):
    pieces, out = refs[:-1], refs[-1]
    for q, piece in enumerate(pieces):
        for r in range(s.rows):
            live = min(max(s.live_x - r * s.width_x, 0), s.width_x)
            if live:
                out[r, q, :live] = piece[r * s.width_x : r * s.width_x + live]
            if live < s.width_x:
                out[r, q, live:] = jnp.zeros((s.width_x - live, 8, s.lanes), F32)


def of_rows(s, pieces):
    return pl.pallas_call(
        functools.partial(spread_kernel, s),
        in_specs=[pl.BlockSpec(memory_space=pltpu.VMEM)] * s.cols,
        out_specs=pl.BlockSpec(memory_space=pltpu.VMEM),
        out_shape=jax.ShapeDtypeStruct((s.rows, s.cols, s.width_x, 8, s.lanes), F32),
        compiler_params=pltpu.CompilerParams(vmem_limit_bytes=VMEM_LIMIT),
        name="spread",
    )(*pieces)


def forward_rows_first(s, field):
    return col_exchange(s, of_cols(s, row_exchange(field)))


def forward_cols_first(s, pieces):
    return of_cols(s, row_exchange(jnp.stack(col_exchange(s, pieces), axis=1)))


def backward_cols_first(s, pieces):
    return row_exchange(of_rows(s, col_exchange(s, pieces)))


def backward_rows_first(s, pieces):
    got = row_exchange(of_rows(s, pieces))
    return jnp.stack(col_exchange(s, [got[:, q] for q in range(s.cols)]), axis=1)


def tiled_body(s, velocity, accumulator, remesh_flag, remesh_shift, viscosity, shear, clock, step):
    y_back, x_back, x_fore, y_fore, z_back, z_fore = constant_tables(s)
    place = jnp.stack([lax.axis_index("row"), lax.axis_index("col")]).astype(jnp.int32)
    ints = jnp.concatenate([place, remesh_flag * remesh_shift])
    floats = jnp.concatenate([shear * clock, shear, viscosity, step])
    v0, v1, v2, sums = head(s, ints, floats, velocity, y_back)

    def grid(pieces):
        return to_grid(s, ints, pieces, z_back, x_back)

    u0 = grid(forward_rows_first(s, v0))
    u2 = grid(forward_cols_first(s, v2))
    u1 = grid(forward_rows_first(s, v1))
    a, kept = products(s, 0, ints, [u0, u2], x_fore, z_fore)
    (f,) = products(s, 2, ints, [u1, u2, *kept], x_fore, z_fore)
    b, c = products(s, 1, ints, [u0, u1, u2], x_fore, z_fore)
    a = backward_cols_first(s, a)
    f = backward_rows_first(s, f)
    b = backward_cols_first(s, b)
    c = backward_cols_first(s, c)
    own = jnp.sum(sums, axis=(2, 3))
    shares = col_exchange(s, [own] * s.cols)
    totals = ((shares[0] + shares[1]) + (shares[2] + shares[3])) / (s.full_y * s.full_z)
    spectra = jnp.stack([totals[:, 0], 2.0 * viscosity[0] * totals[:, 1]])
    state = update(s, early_kernel, ints, floats, velocity, accumulator, (a, b), y_fore, {})
    state = update(s, late_kernel, ints, floats, *state, (c, f), y_fore, {2: 0, 3: 1})
    return (*state, spectra)


def solution(mesh):
    in_specs = (
        P(None, None, "row", "col", None),
        P(None, None, "row", "col", None),
        P("row"),
        P("row"),
        P(),
        P(),
        P(),
        P(),
    )
    out_specs = (
        P(None, None, "row", "col", None),
        P(None, None, "row", "col", None),
        P(None, "row"),
    )
    rows, cols = mesh.shape["row"], mesh.shape["col"]

    def local(velocity, *rest):
        s = Sizes(rows, cols, velocity.shape[2], velocity.shape[3], velocity.shape[4])
        run = functools.partial(tiled_body, s) if s.fits() else body
        return run(velocity, *rest)

    return jax.shard_map(local, mesh=mesh, in_specs=in_specs, out_specs=out_specs, check_vma=False)
```

```python
import functools
import math

import jax
import jax.numpy as jnp
import numpy as np
from jax import lax
from jax.experimental import pallas as pl
from jax.experimental.pallas import tpu as pltpu
from jax.sharding import PartitionSpec as P


F32 = jnp.float32
BF16 = jnp.bfloat16
ROWS_A_STEP = 8
VMEM_LIMIT = 56 * 1024 * 1024


def signed_index(positions, period):
    return jnp.where(2 * positions < period, positions, positions - period)


def roll_rows(field, amounts):

    def shift_row(row_data, amount_one):
        return jnp.roll(row_data, -amount_one, axis=-1)

    return jax.vmap(shift_row, in_axes=(2, 0), out_axes=2)(field, amounts)


def dft_tables(period):
    positions = jnp.arange(period, dtype=jnp.int32)
    product = positions[:, None] * positions[None, :] % period
    angles = product.astype(jnp.float32) * (2.0 * math.pi / period)
    factor = 1.0 / math.sqrt(period)
    return (jnp.cos(angles) * factor, jnp.sin(angles) * factor)


def product_high(formula, first_arg, second_arg):
    return jnp.einsum(formula, first_arg, second_arg, precision=lax.Precision.HIGHEST)


def rotate(left_side, right_side, output, real_part, imag_part, cosine_table, sine_table, backward):
    stacked = jnp.stack([real_part, imag_part])
    if backward:
        block_table = jnp.stack(
            [jnp.stack([cosine_table, sine_table]), jnp.stack([-sine_table, cosine_table])]
        )
    else:
        block_table = jnp.stack(
            [jnp.stack([cosine_table, -sine_table]), jnp.stack([sine_table, cosine_table])]
        )
    result = product_high(
        "s" + left_side + ",st" + right_side + "->t" + output, stacked, block_table
    )
    return (result[0], result[1])


def project(real_part, imag_part, wave_vector, inverse_square):
    along_real = (
        wave_vector[0] * real_part[0]
        + wave_vector[1] * real_part[1]
        + wave_vector[2] * real_part[2]
    ) * inverse_square
    along_imag = (
        wave_vector[0] * imag_part[0]
        + wave_vector[1] * imag_part[1]
        + wave_vector[2] * imag_part[2]
    ) * inverse_square
    return (
        jnp.stack([real_part[number] - wave_vector[number] * along_real for number in range(3)]),
        jnp.stack([imag_part[number] - wave_vector[number] * along_imag for number in range(3)]),
    )


def cross_product(first_one, second_one):
    return jnp.stack(
        [
            first_one[1] * second_one[2] - first_one[2] * second_one[1],
            first_one[2] * second_one[0] - first_one[0] * second_one[2],
            first_one[0] * second_one[1] - first_one[1] * second_one[0],
        ]
    )


def to_physical(real_part, imag_part, tables_all):
    (cos_y, sin_y), (cos_x, sin_x), (cos_z, sin_z) = tables_all
    row_count = lax.axis_size("row")
    col_count = lax.axis_size("col")
    fields, width_x, width_z, full_y = real_part.shape
    block_y = full_y // row_count
    half_x = width_x * row_count
    full_x = cos_x.shape[0]
    block_x = full_x // col_count
    full_z = width_z * col_count
    shape_y = (full_y, row_count, block_y)
    first_real, first_imag = rotate(
        "fabc",
        "cpq",
        "fpabq",
        real_part,
        imag_part,
        cos_y.reshape(shape_y),
        sin_y.reshape(shape_y),
        True,
    )
    flat_shape = (fields, row_count, width_x, width_z * block_y)
    second_real, second_imag = (
        lax.all_to_all(
            first_real.reshape(flat_shape), "row", split_axis=1, concat_axis=2, tiled=True
        ),
        lax.all_to_all(
            first_imag.reshape(flat_shape), "row", split_axis=1, concat_axis=2, tiled=True
        ),
    )
    deep_shape = (fields, half_x, width_z, block_y)
    weights = jnp.where(jnp.arange(half_x) == 0, 1.0, 2.0).astype(jnp.float32)[:, None]
    shape_x = (half_x, col_count, block_x)
    cos_half = (weights * cos_x[:half_x]).reshape(shape_x)
    sin_half = (weights * sin_x[:half_x]).reshape(shape_x)
    third_real, third_imag = rotate(
        "fkzy",
        "kpq",
        "fpzyq",
        second_real.reshape(deep_shape),
        second_imag.reshape(deep_shape),
        cos_half,
        sin_half,
        True,
    )
    flat_shape = (fields, col_count, 1, width_z * block_y * block_x)
    fourth_real, fourth_imag = (
        lax.all_to_all(
            third_real.reshape(flat_shape), "col", split_axis=1, concat_axis=2, tiled=True
        ),
        lax.all_to_all(
            third_imag.reshape(flat_shape), "col", split_axis=1, concat_axis=2, tiled=True
        ),
    )
    deep_shape = (fields, col_count, width_z, block_y, block_x)
    shape_z = (col_count, width_z, full_z)
    stacked = jnp.stack([fourth_real.reshape(deep_shape), fourth_imag.reshape(deep_shape)])
    z_table = jnp.stack([cos_z.reshape(shape_z), -sin_z.reshape(shape_z)])
    return product_high("sfpkyq,spkn->fyqn", stacked, z_table)


def to_spectral(physical, tables_all, half_x):
    (cos_y, sin_y), (cos_x, sin_x), (cos_z, sin_z) = tables_all
    row_count = lax.axis_size("row")
    col_count = lax.axis_size("col")
    fields, block_y, block_x, full_z = physical.shape
    width_z = full_z // col_count
    width_x = half_x // row_count
    full_y = block_y * row_count
    shape_z = (full_z, col_count, width_z)
    z_table = jnp.stack([cos_z.reshape(shape_z), -sin_z.reshape(shape_z)])
    first_both = product_high("fyqn,tnpk->tfpkyq", physical, z_table)
    first_real, first_imag = (first_both[0], first_both[1])
    flat_shape = (fields, col_count, 1, width_z * block_y * block_x)
    second_real, second_imag = (
        lax.all_to_all(
            first_real.reshape(flat_shape), "col", split_axis=1, concat_axis=2, tiled=True
        ),
        lax.all_to_all(
            first_imag.reshape(flat_shape), "col", split_axis=1, concat_axis=2, tiled=True
        ),
    )
    deep_shape = (fields, col_count, width_z, block_y, block_x)
    shape_x = (col_count, block_x, row_count, width_x)
    third_real, third_imag = rotate(
        "fpkyq",
        "pqmr",
        "fmrky",
        second_real.reshape(deep_shape),
        second_imag.reshape(deep_shape),
        cos_x[:, :half_x].reshape(shape_x),
        sin_x[:, :half_x].reshape(shape_x),
        False,
    )
    flat_shape = (fields, row_count, 1, width_x * width_z * block_y)
    fourth_real, fourth_imag = (
        lax.all_to_all(
            third_real.reshape(flat_shape), "row", split_axis=1, concat_axis=2, tiled=True
        ),
        lax.all_to_all(
            third_imag.reshape(flat_shape), "row", split_axis=1, concat_axis=2, tiled=True
        ),
    )
    deep_shape = (fields, row_count, width_x, width_z, block_y)
    shape_y = (row_count, block_y, full_y)
    return rotate(
        "fparq",
        "pqn",
        "farn",
        fourth_real.reshape(deep_shape),
        fourth_imag.reshape(deep_shape),
        cos_y.reshape(shape_y),
        sin_y.reshape(shape_y),
        False,
    )


def many_physical(real_part, imag_part, tables_all):
    return jnp.concatenate(
        [
            to_physical(real_part[number : number + 1], imag_part[number : number + 1], tables_all)
            for number in range(real_part.shape[0])
        ]
    )


def many_spectral(physical, tables_all, half_x):
    result_list = [
        to_spectral(physical[number : number + 1], tables_all, half_x)
        for number in range(physical.shape[0])
    ]
    return (
        jnp.concatenate([entry[0] for entry in result_list]),
        jnp.concatenate([entry[1] for entry in result_list]),
    )


def body(velocity, accumulator, remesh_flag, remesh_shift, viscosity, shear, clock, step):
    width_x = velocity.shape[2]
    width_z = velocity.shape[3]
    full_y = velocity.shape[4]
    half_x = width_x * lax.axis_size("row")
    NX, NY, NZ = 2 * half_x, full_y, width_z * lax.axis_size("col")
    offset = remesh_flag * remesh_shift
    remeshed = roll_rows(velocity, offset)
    carried = roll_rows(accumulator, offset)
    lattice_x = lax.axis_index("row") * width_x + jnp.arange(width_x, dtype=jnp.int32)
    col_index = lax.axis_index("col") * width_z + jnp.arange(width_z, dtype=jnp.int32)
    lattice_z = signed_index(col_index, NZ)
    lattice_y = signed_index(jnp.arange(full_y, dtype=jnp.int32), NY)
    wave_x = lattice_x.astype(jnp.float32)[:, None, None]
    wave_z = lattice_z.astype(jnp.float32)[None, :, None]
    wave_y = lattice_y.astype(jnp.float32)[None, None, :] - shear[0] * clock[0] * wave_x
    wave_vector = (wave_x, wave_y, wave_z)
    square_wave = wave_x * wave_x + wave_y * wave_y + wave_z * wave_z
    inverse_square = 1.0 / jnp.maximum(square_wave, 1.0)
    dealias_mask = (
        (3 * lattice_x < NX)[:, None, None]
        & (3 * jnp.abs(lattice_z) < NZ)[None, :, None]
        & (3 * jnp.abs(lattice_y) < NY)[None, None, :]
    ).astype(jnp.float32)
    shear_rate = shear[0]
    viscous_rate = viscosity[0]
    stress_part = jnp.sum(
        remeshed[0, 0] * remeshed[1, 0] + remeshed[0, 1] * remeshed[1, 1], axis=(1, 2)
    )
    energy = jnp.sum(remeshed * remeshed, axis=(0, 1))
    dissipation_part = jnp.sum(square_wave * energy, axis=(1, 2))
    stress_total, dissipation_total = lax.psum((stress_part, dissipation_part), "col")
    solen_real, solen_imag = project(remeshed[:, 0], remeshed[:, 1], wave_vector, inverse_square)
    smooth_real = dealias_mask * solen_real
    smooth_imag = dealias_mask * solen_imag
    tables_all = (dft_tables(NY), dft_tables(NX), dft_tables(NZ))
    vort_real = -cross_product(wave_vector, smooth_imag)
    vort_imag = cross_product(wave_vector, smooth_real)
    both_real = jnp.concatenate([smooth_real, vort_real])
    both_imag = jnp.concatenate([smooth_imag, vort_imag])
    physical = many_physical(both_real, both_imag, tables_all)
    lamb_grid = cross_product(physical[:3], physical[3:])
    modes_real, modes_imag = many_spectral(lamb_grid, tables_all, half_x)
    hat_real = dealias_mask * modes_real
    hat_imag = dealias_mask * modes_imag
    proj_real, proj_imag = project(hat_real, hat_imag, wave_vector, inverse_square)
    coupling = 2.0 * shear_rate * wave_x * inverse_square

    def tendency(projected, state):
        term_list = [
            projected[number]
            + coupling * wave_vector[number] * state[1]
            - viscous_rate * square_wave * state[number]
            for number in range(3)
        ]
        term_list[0] = term_list[0] - shear_rate * state[1]
        return jnp.stack(term_list)

    tendencies = jnp.stack(
        [tendency(proj_real, remeshed[:, 0]), tendency(proj_imag, remeshed[:, 1])], axis=1
    )
    new_accumulator = -5.0 / 9.0 * carried + step[0] * tendencies
    new_velocity = remeshed + 15.0 / 16.0 * new_accumulator
    stress = stress_total / (NY * NZ)
    dissipation = 2.0 * viscous_rate * dissipation_total / (NY * NZ)
    return (new_velocity, new_accumulator, jnp.stack([stress, dissipation]))


def angle(rows, cols, n):
    product = np.outer(rows, cols) % n
    return np.cos(2 * np.pi * product / n) / math.sqrt(n), np.sin(2 * np.pi * product / n) / math.sqrt(n)


def halves(table):
    table = np.asarray(table, np.float32)
    high = table.astype(jnp.bfloat16)
    low = (table - high.astype(np.float32)).astype(jnp.bfloat16)
    return high, low


def split(x):
    high = x.astype(BF16)
    return high, (x - high.astype(F32)).astype(BF16)


def dot(a, b, dims):
    return lax.dot_general(a, b, (dims, ((), ())), preferred_element_type=F32)


class Sizes:
    def __init__(self, rows, cols, width_x, width_z, full_y):
        self.rows, self.cols = rows, cols
        self.width_x, self.width_z = width_x, width_z
        self.half_x = width_x * rows
        self.full_x = 2 * self.half_x
        self.full_z = width_z * cols
        self.full_y = full_y
        self.block_y = full_y // (rows * cols)
        live = (self.full_x - 1) // 3 + 1
        self.live_x = -(-live // 8) * 8
        self.lanes = 2 * width_z

    def fits(self):
        return (
            self.block_y == 8
            and self.cols == 4
            and self.lanes == 128
            and self.full_y % 128 == 0
            and self.full_z % 128 == 0
            and self.full_x % 128 == 0
            and self.width_x % ROWS_A_STEP == 0
            and self.rows & (self.rows - 1) == 0
            and self.cols & (self.cols - 1) == 0
        )


def constant_tables(s):
    c, n = angle(np.arange(s.full_y), np.arange(s.full_y), s.full_y)
    y_back = np.concatenate([c, -n], axis=1)
    y_fore = np.concatenate([c, n], axis=1)
    live = np.arange(s.live_x)
    weight = np.where(live == 0, 1.0, 2.0) * (3 * live < s.full_x)
    c, n = angle(np.arange(s.full_x), live, s.full_x)
    x_back = np.concatenate([c * weight, -n * weight], axis=1)
    x_fore = np.concatenate([c.T, -n.T], axis=0)
    c, n = angle(np.arange(s.full_z), np.arange(s.full_z), s.full_z)
    c3, n3 = c.reshape(s.cols, s.width_z, s.full_z), n.reshape(s.cols, s.width_z, s.full_z)
    z_back = np.concatenate(
        [np.concatenate([c3, n3], axis=2), np.concatenate([-n3, c3], axis=2)], axis=1
    )
    ct, nt = c3.transpose(0, 2, 1), n3.transpose(0, 2, 1)
    z_fore = np.concatenate(
        [np.concatenate([ct, -nt], axis=2), np.concatenate([nt, ct], axis=2)], axis=1
    )
    left = [np.concatenate(halves(t), axis=0) for t in (y_back, x_back, x_fore)]
    return left + [halves(t) for t in (y_fore, z_back, z_fore)]


def by_left_table(table, rows, high, low, inner):
    out = dot(table[...], high, inner)
    return out[:rows] + (out[rows:] + dot(table[:rows], low, inner))


def by_right_table(data, high, low):
    n = data.shape[0]
    top, rest = split(data)
    out = dot(jnp.concatenate([top, rest], axis=0), high, ((1,), (0,)))
    return out[:n] + (out[n:] + dot(top, low, ((1,), (0,))))


def whole(shape):
    return pl.BlockSpec(shape, lambda *_: (0,) * len(shape))


def waves(s, kx, col, shear_clock):
    plane = (s.width_z, s.full_y)
    iz = lax.broadcasted_iota(jnp.int32, plane, 0) + col * s.width_z
    iz = jnp.where(2 * iz < s.full_z, iz, iz - s.full_z)
    iy = lax.broadcasted_iota(jnp.int32, plane, 1)
    iy = jnp.where(2 * iy < s.full_y, iy, iy - s.full_y)
    k0 = kx.astype(F32)
    k1 = iy.astype(F32) - shear_clock * k0
    k2 = iz.astype(F32)
    ksq = k0 * k0 + k1 * k1 + k2 * k2
    inverse = 1.0 / jnp.maximum(ksq, 1.0)
    inside = (3 * jnp.abs(iz) < s.full_z) & (3 * jnp.abs(iy) < s.full_y) & (3 * kx < s.full_x)
    return k0, k1, k2, ksq, inverse, inside.astype(F32)


def rolled(s, ref, j, amount):
    flat = jnp.concatenate([ref[c, p, j] for c in range(3) for p in range(2)], axis=0)
    flat = pltpu.roll(flat, lax.rem(s.full_y - amount, s.full_y), 1)
    w = s.width_z
    return [[flat[(2 * c + p) * w : (2 * c + p + 1) * w] for p in range(2)] for c in range(3)]


def head_kernel(s, ints, floats, vel, table, *outs):
    fields, sums, made = outs[:-2], outs[-2], outs[-1]
    row, col = ints[0], ints[1]
    step = pl.program_id(0)
    right = [[], [], []]
    for j in range(2):
        local = 2 * step + j
        kx = row * s.width_x + local
        v = rolled(s, vel, j, ints[2 + local])
        k0, k1, k2, ksq, inverse, mask = waves(s, kx, col, floats[0])
        stress = v[0][0] * v[1][0] + v[0][1] * v[1][1]
        energy = sum(v[c][p] * v[c][p] for c in range(3) for p in range(2))
        fold = lambda a: jnp.sum(a.reshape(s.width_z // 8, 8, s.full_y), axis=0)
        sums[j, 0] = fold(stress)
        sums[j, 1] = fold(ksq * energy)
        along = [(k0 * v[0][p] + k1 * v[1][p] + k2 * v[2][p]) * inverse for p in range(2)]
        for c, k in enumerate((k0, k1, k2)):
            (rh, rl), (ih, il) = [split(mask * (v[c][p] - k * along[p])) for p in range(2)]
            right[c].append([jnp.concatenate([rh, ih], axis=1), jnp.concatenate([rl, il], axis=1)])
            right[c].append([jnp.concatenate([ih, -rh], axis=1), jnp.concatenate([il, -rl], axis=1)])
    for c in range(3):
        high, low = [jnp.concatenate([x[i] for x in right[c]], axis=0) for i in range(2)]
        made[...] = by_left_table(table, s.full_y, high, low, ((1,), (1,)))
        for r in range(s.rows):
            for q in range(s.cols):
                at = pl.multiple_of((r * s.cols + (q ^ col)) * 8, 8)
                for j in range(2):
                    tile = made[pl.ds(at, 8), j * 128 : (j + 1) * 128]
                    fields[c][r, q, j] = tile


def head(s, ints, floats, velocity, table):
    out = pl.pallas_call(
        functools.partial(head_kernel, s),
        grid=(s.width_x // 2,),
        in_specs=[
            pl.BlockSpec(memory_space=pltpu.SMEM),
            pl.BlockSpec(memory_space=pltpu.SMEM),
            pl.BlockSpec((3, 2, 2, s.width_z, s.full_y), lambda i: (0, 0, i, 0, 0)),
            whole(table.shape),
        ],
        out_specs=[pl.BlockSpec((s.rows, s.cols, 2, 8, s.lanes), lambda i: (0, 0, i, 0, 0))] * 3
        + [pl.BlockSpec((2, 2, 8, s.full_y), lambda i: (i, 0, 0, 0))],
        out_shape=[jax.ShapeDtypeStruct((s.rows, s.cols, s.width_x, 8, s.lanes), F32)] * 3
        + [jax.ShapeDtypeStruct((s.width_x, 2, 8, s.full_y), F32)],
        scratch_shapes=[pltpu.VMEM((s.full_y, 256), F32)],
        compiler_params=pltpu.CompilerParams(vmem_limit_bytes=VMEM_LIMIT),
        name="head",
    )(ints, floats, velocity, table)
    return out


def grid_kernel(s, ints, *refs):
    pieces, (zh, zl, x_table, out, mid) = refs[: s.cols], refs[s.cols :]
    col = ints[1]
    rows = s.live_x * 8
    step = rows // 2
    high_z = jnp.concatenate([zh[q ^ col] for q in range(s.cols)], axis=0)
    low_z = jnp.concatenate([zl[q ^ col] for q in range(s.cols)], axis=0)

    def along_z(i, carry):
        at = pl.multiple_of(i * (step // 8), step // 8)
        parts = [p[pl.ds(at, step // 8)].reshape(step, s.lanes) for p in pieces]
        full = by_right_table(jnp.concatenate(parts, axis=1), high_z, low_z)
        for t in range(2 * s.full_z // 128):
            mid[t, pl.ds(pl.multiple_of(i * step, step), step)] = full[:, t * 128 : (t + 1) * 128]
        return carry

    lax.fori_loop(0, 2, along_z, 0)

    def along_x(y, carry):
        tiles = [mid[t, pl.ds(y, s.live_x, stride=8)] for t in range(2 * s.full_z // 128)]
        half = s.full_z // 128
        both = [jnp.concatenate(tiles[:half], axis=1), jnp.concatenate(tiles[half:], axis=1)]
        high, low = split(jnp.concatenate(both, axis=0))
        out[y] = by_left_table(x_table, s.full_x, high, low, ((1,), (0,)))
        return carry

    lax.fori_loop(0, 8, along_x, 0)


def to_grid(s, ints, pieces, z_table, x_table):
    rows = s.live_x * 8
    return pl.pallas_call(
        functools.partial(grid_kernel, s),
        in_specs=[pl.BlockSpec(memory_space=pltpu.SMEM)]
        + [pl.BlockSpec(memory_space=pltpu.VMEM)] * (s.cols + 3),
        out_specs=pl.BlockSpec(memory_space=pltpu.VMEM),
        out_shape=jax.ShapeDtypeStruct((8, s.full_x, s.full_z), F32),
        scratch_shapes=[pltpu.VMEM((2 * s.full_z // 128, rows, 128), F32)],
        compiler_params=pltpu.CompilerParams(vmem_limit_bytes=VMEM_LIMIT),
        name="to_grid",
    )(ints, *pieces, *z_table, x_table)


def turn(s, rows, base, kz):
    k0 = ((lax.broadcasted_iota(jnp.int32, (rows, s.lanes), 0) + base) // 8).astype(F32)
    square = k0 * k0 + kz * kz
    scale = lax.rsqrt(jnp.maximum(square, 1.0))
    return jnp.where(square > 0, k0 * scale, 1.0), kz * scale


def back_kernel(s, which, ints, *refs):
    given, _, made = BACK[which]
    u, refs = refs[:given], refs[given:]
    saved, refs = (refs[: s.cols], refs[s.cols :]) if which == 2 else (None, refs)
    (x_table, zh, zl), refs = refs[:3], refs[3:]
    outs, mids = refs[: made * s.cols], refs[made * s.cols :]
    col = ints[1]

    def along_x(y, carry):
        w = [ref[y] for ref in u]
        if which == 0:
            terms = [w[0] * w[0] - w[1] * w[1], w[0] * w[1]]
        elif which == 1:
            terms = [w[0] * w[1], w[1] * w[2]]
        else:
            terms = [w[0] * w[0] - w[1] * w[1]]
        for mid, term in zip(mids, terms):
            high, low = split(term)
            out = by_left_table(x_table, 2 * s.live_x, high, low, ((1,), (0,)))
            half = s.full_z // 128
            for t in range(2 * half):
                p, at = t // half, (t % half) * 128
                tile = out[p * s.live_x : (p + 1) * s.live_x, at : at + 128]
                mid[t, pl.ds(y, s.live_x, stride=8)] = tile
        return carry

    lax.fori_loop(0, 8, along_x, 0)
    rows = s.live_x * 8
    step = rows // 2
    high_z = jnp.concatenate([zh[q ^ col] for q in range(s.cols)], axis=1)
    low_z = jnp.concatenate([zl[q ^ col] for q in range(s.cols)], axis=1)

    def along_z(i, carry):
        at = pl.multiple_of(i * step, step)
        done = []
        for mid in mids:
            data = [mid[t, pl.ds(at, step)] for t in range(2 * s.full_z // 128)]
            done.append(by_right_table(jnp.concatenate(data, axis=1), high_z, low_z))
        here = pl.ds(pl.multiple_of(i * (step // 8), step // 8), step // 8)
        shape = (step // 8, 8, s.lanes)
        for q in range(s.cols):
            part = [d[:, q * s.lanes : (q + 1) * s.lanes] for d in done]
            if which == 2:
                outs[q][here] = part[0].reshape(shape) - saved[q][here]
                continue
            lane = lax.broadcasted_iota(jnp.int32, (step, s.lanes), 1)
            iz = lax.rem(lane, s.width_z) + (q ^ col) * s.width_z
            kz = jnp.where(2 * iz < s.full_z, iz, iz - s.full_z).astype(F32)
            cosine, sine = turn(s, step, i * step, kz)
            if which == 0:
                first = cosine * sine * part[0] + (sine * sine - cosine * cosine) * part[1]
                second = cosine * (cosine * part[0] + 2.0 * sine * part[1])
            else:
                first = sine * part[0] - cosine * part[1]
                second = cosine * part[0] + sine * part[1]
            outs[q][here] = first.reshape(shape)
            outs[s.cols + q][here] = second.reshape(shape)
        return carry

    lax.fori_loop(0, 2, along_z, 0)


BACK = ((2, 2, 2), (3, 2, 2), (2, 1, 1))


def products(s, which, ints, fields, x_table, z_table):
    rows = s.live_x * 8
    _, number, made = BACK[which]
    piece = jax.ShapeDtypeStruct((s.live_x, 8, s.lanes), F32)
    out = pl.pallas_call(
        functools.partial(back_kernel, s, which),
        in_specs=[pl.BlockSpec(memory_space=pltpu.SMEM)]
        + [pl.BlockSpec(memory_space=pltpu.VMEM)] * (len(fields) + 3),
        out_specs=[pl.BlockSpec(memory_space=pltpu.VMEM)] * (made * s.cols),
        out_shape=[piece] * (made * s.cols),
        scratch_shapes=[pltpu.VMEM((2 * s.full_z // 128, rows, 128), F32)] * number,
        compiler_params=pltpu.CompilerParams(vmem_limit_bytes=VMEM_LIMIT),
    )(ints, *fields, x_table, *z_table)
    return [out[i * s.cols : (i + 1) * s.cols] for i in range(made)]


def frame(s, kx, col, shear_clock):
    k0, k1, k2, ksq, inverse, mask = waves(s, kx, col, shear_clock)
    flat = k0 * k0 + k2 * k2
    scale = lax.rsqrt(jnp.maximum(flat, 1.0))
    cosine, sine = jnp.where(flat > 0, k0 * scale, 1.0), k2 * scale
    return (k0, k1, k2), ksq, inverse, mask, flat, flat * scale, cosine, sine


def modes_of(s, j, col, refs, yh, yl):
    turned = []
    for ref in refs:
        tiles = [ref[r, q ^ col, j] for r in range(s.rows) for q in range(s.cols)]
        turned.append(jnp.concatenate(tiles, axis=0).T)
    every = by_right_table(jnp.concatenate(turned, axis=0), yh[...], yl[...])
    modes = []
    w, n = s.width_z, s.full_y
    for i in range(len(refs)):
        both = every[i * s.lanes : (i + 1) * s.lanes]
        modes.append((both[:w, :n] + both[w:, n:], both[w:, :n] - both[:w, n:]))
    return modes


def early_row(s, j, ints, floats, vel, acc, fa, fb, yh, yl, new_vel, new_acc):
    row, col = ints[0], ints[1]
    local = ROWS_A_STEP * pl.program_id(0) + j
    kx, amount = row * s.width_x + local, ints[2 + local]
    modes = modes_of(s, j, col, (fa, fb), yh, yl)
    k, ksq, inverse, mask, _, kh, cosine, sine = frame(s, kx, col, floats[0])
    v = rolled(s, vel, j, amount)
    old = rolled(s, acc, j, amount)
    shear, viscosity, dt = floats[1], floats[2], floats[3]
    coupling = (2.0 * shear) * k[0] * inverse
    for p in range(2):
        a, b = [m[1 - p] for m in modes]
        qt = (kh * a + k[1] * b) * (mask if p == 0 else -mask)
        nonlinear = (qt * sine, None, -(qt * cosine))
        drive = coupling * v[1][p]
        for c3 in range(3):
            rate = k[c3] * drive - (viscosity * ksq) * v[c3][p]
            if c3 != 1:
                rate = rate + nonlinear[c3]
            if c3 == 0:
                rate = rate - shear * v[1][p]
            fresh = (-5.0 / 9.0) * old[c3][p] + dt * rate
            new_acc[c3, p, j] = fresh
            new_vel[c3, p, j] = v[c3][p] + (15.0 / 16.0) * fresh


def late_row(s, j, ints, floats, vel, acc, fc, ff, yh, yl, new_vel, new_acc):
    row, col = ints[0], ints[1]
    kx = row * s.width_x + ROWS_A_STEP * pl.program_id(0) + j
    modes = modes_of(s, j, col, (fc, ff), yh, yl)
    k, _, inverse, mask, flat, kh, cosine, sine = frame(s, kx, col, floats[0])
    dt = floats[3] * mask
    lean = dt * (flat - k[1] * k[1]) * inverse
    cross = dt * kh * k[1] * inverse
    for p in range(2):
        c, f = [m[1 - p] for m in modes]
        qe = lean * c + cross * f
        if p == 1:
            qe = -qe
        slope = qe * k[1]
        for c3, add in enumerate((-(slope * cosine), qe * kh, -(slope * sine))):
            new_acc[c3, p, j] = acc[c3, p, j] + add
            new_vel[c3, p, j] = vel[c3, p, j] + (15.0 / 16.0) * add


def each_row(one, s, *refs):
    for j in range(ROWS_A_STEP):
        one(s, j, *refs)


early_kernel = functools.partial(each_row, early_row)
late_kernel = functools.partial(each_row, late_row)


def update(s, kernel, ints, floats, velocity, accumulator, fields, table, alias):
    n = ROWS_A_STEP
    plane = pl.BlockSpec((3, 2, n, s.width_z, s.full_y), lambda i: (0, 0, i, 0, 0))
    piece = pl.BlockSpec((s.rows, s.cols, n, 8, s.lanes), lambda i: (0, 0, i, 0, 0))
    y2 = (s.full_y, 2 * s.full_y)
    shape = jax.ShapeDtypeStruct(velocity.shape, F32)
    return pl.pallas_call(
        functools.partial(kernel, s),
        grid=(s.width_x // n,),
        in_specs=[pl.BlockSpec(memory_space=pltpu.SMEM)] * 2
        + [plane] * 2
        + [piece] * 2
        + [whole(y2)] * 2,
        out_specs=[plane] * 2,
        out_shape=[shape] * 2,
        input_output_aliases=alias,
        compiler_params=pltpu.CompilerParams(vmem_limit_bytes=VMEM_LIMIT),
    )(ints, floats, velocity, accumulator, *fields, *table)


def col_exchange(s, pieces):
    out = [pieces[0]]
    for q in range(1, s.cols):
        out.append(lax.ppermute(pieces[q], "col", [(i, i ^ q) for i in range(s.cols)]))
    return out


def row_exchange(field):
    return lax.all_to_all(field, "row", 0, 0, tiled=True)


def of_cols(s, got):
    return [got[:, q].reshape(s.half_x, 8, s.lanes)[: s.live_x] for q in range(s.cols)]


def spread_kernel(s, *refs):
    pieces, out = refs[:-1], refs[-1]
    for q, piece in enumerate(pieces):
        for r in range(s.rows):
            live = min(max(s.live_x - r * s.width_x, 0), s.width_x)
            if live:
                out[r, q, :live] = piece[r * s.width_x : r * s.width_x + live]
            if live < s.width_x:
                out[r, q, live:] = jnp.zeros((s.width_x - live, 8, s.lanes), F32)


def of_rows(s, pieces):
    return pl.pallas_call(
        functools.partial(spread_kernel, s),
        in_specs=[pl.BlockSpec(memory_space=pltpu.VMEM)] * s.cols,
        out_specs=pl.BlockSpec(memory_space=pltpu.VMEM),
        out_shape=jax.ShapeDtypeStruct((s.rows, s.cols, s.width_x, 8, s.lanes), F32),
        compiler_params=pltpu.CompilerParams(vmem_limit_bytes=VMEM_LIMIT),
        name="spread",
    )(*pieces)


def forward_rows_first(s, field):
    return col_exchange(s, of_cols(s, row_exchange(field)))


def backward_cols_first(s, pieces):
    return row_exchange(of_rows(s, col_exchange(s, pieces)))


def backward_rows_first(s, pieces):
    got = row_exchange(of_rows(s, pieces))
    return jnp.stack(col_exchange(s, [got[:, q] for q in range(s.cols)]), axis=1)


def tiled_body(s, velocity, accumulator, remesh_flag, remesh_shift, viscosity, shear, clock, step):
    y_back, x_back, x_fore, y_fore, z_back, z_fore = constant_tables(s)
    place = jnp.stack([lax.axis_index("row"), lax.axis_index("col")]).astype(jnp.int32)
    ints = jnp.concatenate([place, remesh_flag * remesh_shift])
    floats = jnp.concatenate([shear * clock, shear, viscosity, step])
    v0, v1, v2, sums = head(s, ints, floats, velocity, y_back)

    def grid(pieces):
        return to_grid(s, ints, pieces, z_back, x_back)

    u0 = grid(forward_rows_first(s, v0))
    u2 = grid(forward_rows_first(s, v2))
    u1 = grid(forward_rows_first(s, v1))
    a, kept = products(s, 0, ints, [u0, u2], x_fore, z_fore)
    (f,) = products(s, 2, ints, [u1, u2, *kept], x_fore, z_fore)
    b, c = products(s, 1, ints, [u0, u1, u2], x_fore, z_fore)
    a = backward_cols_first(s, a)
    f = backward_rows_first(s, f)
    b = backward_cols_first(s, b)
    c = backward_cols_first(s, c)
    own = jnp.sum(sums, axis=(2, 3))
    shares = col_exchange(s, [own] * s.cols)
    totals = ((shares[0] + shares[1]) + (shares[2] + shares[3])) / (s.full_y * s.full_z)
    spectra = jnp.stack([totals[:, 0], 2.0 * viscosity[0] * totals[:, 1]])
    state = update(s, early_kernel, ints, floats, velocity, accumulator, (a, b), y_fore, {})
    state = update(s, late_kernel, ints, floats, *state, (c, f), y_fore, {2: 0, 3: 1})
    return (*state, spectra)


def solution(mesh):
    in_specs = (
        P(None, None, "row", "col", None),
        P(None, None, "row", "col", None),
        P("row"),
        P("row"),
        P(),
        P(),
        P(),
        P(),
    )
    out_specs = (
        P(None, None, "row", "col", None),
        P(None, None, "row", "col", None),
        P(None, "row"),
    )
    rows, cols = mesh.shape["row"], mesh.shape["col"]

    def local(velocity, *rest):
        s = Sizes(rows, cols, velocity.shape[2], velocity.shape[3], velocity.shape[4])
        run = functools.partial(tiled_body, s) if s.fits() else body
        return run(velocity, *rest)

    return jax.shard_map(local, mesh=mesh, in_specs=in_specs, out_specs=out_specs, check_vma=False)
```
